16 devices in a mesh: dp: 4 (over y, z, core), sp: 4 (over x).
Axes of the slice: x: 4, y: 2, z: 1, core: 2. Of those that a mesh axis runs over, the one named last changes fastest.
The devices are a block of a 4x4x8 slice.
Arguments:
- x: bfloat16 [8192, 3584], P(('dp', 'sp')), parts along dimension 0
- gain: bfloat16 [3584], replicated
- wq: bfloat16 [3584, 4096], replicated
- wk: bfloat16 [3584, 2048], replicated
- wv: bfloat16 [3584, 2048], replicated
- wo: bfloat16 [4096, 3584], replicated
Outputs:
- output: bfloat16 [8192, 3584], P(('dp', 'sp')), parts along dimension 0
There are 4 independent parts. The reference program is written for one: setup_inputs(seed, part) draws one part's arguments, and reference() takes and returns one part's arrays. A program takes and returns all parts, laid end to end along the dimension named above; an argument that names none is the same for every part.
All inputs are finite; a program needn't handle non-finite values.
Results may differ from the reference program's by a relative error of at most 0.012.
Values are sent between devices in bfloat16 or wider.
A program may use at most 768 MiB of HBM per device.

```python
import jax
import jax.numpy as jnp
from jax import lax

ROWS = 2048
D = 3584
HEADS = 16
KV_HEADS = 8
HEAD = 256
THETA = 10000


def setup_inputs(seed: int = 0, part: int = 0) -> dict:
    kx, kn, kq, kk, kv, ko = jax.random.split(jax.random.key(seed), 6)

    def weights(key, rows, columns):
        return jax.random.normal(key, (rows, columns), jnp.float32) * rows**-0.5

    drawn = {
        "x": jax.random.normal(jax.random.fold_in(kx, part), (ROWS, D), jnp.float32),
        "gain": 1 + 0.1 * jax.random.normal(kn, (D,), jnp.float32),
        "wq": 2 * weights(kq, D, HEADS * HEAD),
        "wk": 2 * weights(kk, D, KV_HEADS * HEAD),
        "wv": 4 * weights(kv, D, KV_HEADS * HEAD),
        "wo": weights(ko, HEADS * HEAD, D),
    }
    return {k: v.astype(jnp.bfloat16) for k, v in drawn.items()}


def normed(x, gain):
    wide = x.astype(jnp.float32)
    scale = lax.rsqrt(jnp.mean(wide * wide, -1, keepdims=True) + 1e-6)
    return (wide * scale * gain.astype(jnp.float32)).astype(jnp.bfloat16)


def turned(t, place, theta):
    half = t.shape[-1] // 2
    angle = place.astype(jnp.float32)[:, None] * theta ** (-jnp.arange(half, dtype=jnp.float32) / half)
    cos, sin = jnp.cos(angle)[:, None], jnp.sin(angle)[:, None]
    a, b = t[..., :half].astype(jnp.float32), t[..., half:].astype(jnp.float32)
    return jnp.concatenate([a * cos - b * sin, b * cos + a * sin], -1).astype(jnp.bfloat16)


def matmul(a, w):
    return jnp.dot(a, w, preferred_element_type=jnp.float32).astype(jnp.bfloat16)


def einsum(form, a, b):
    return jnp.einsum(form, a.astype(jnp.float32), b.astype(jnp.float32))


def attention(q, k, v):
    scores = einsum("tgsd,ugd->gstu", q, k) * q.shape[-1] ** -0.5
    token = jnp.arange(q.shape[0])
    scores = jnp.where(token[:, None] >= token, scores, -jnp.inf)
    weights = jax.nn.softmax(scores, -1).astype(jnp.bfloat16)
    return einsum("gstu,ugd->tgsd", weights, v).astype(jnp.bfloat16)


def reference(x, gain, wq, wk, wv, wo):
    a, place = normed(x, gain), jnp.arange(ROWS)
    q = turned(matmul(a, wq).reshape(ROWS, HEADS, HEAD), place, THETA).reshape(ROWS, KV_HEADS, -1, HEAD)
    k = turned(matmul(a, wk).reshape(ROWS, KV_HEADS, HEAD), place, THETA)
    v = matmul(a, wv).reshape(ROWS, KV_HEADS, HEAD)
    seen = attention(q, k, v).reshape(ROWS, HEADS * HEAD)
    return (x.astype(jnp.float32) + jnp.dot(seen, wo, preferred_element_type=jnp.float32)).astype(jnp.bfloat16)
```

```python
import functools

import jax
import jax.numpy as jnp
import numpy as np
from jax import lax
from jax.experimental import pallas as pl
from jax.experimental.pallas import tpu as pltpu
from jax.sharding import PartitionSpec as P

HEAD = 256
THETA = 10000
HIDDEN = -2e30
LOG2E = 1.4426950408889634
MESH = pl.DeviceIdType.MESH
LEAD = 3
F32, BF16 = jnp.float32, jnp.bfloat16


def _dot(a, b):
    return lax.dot_general(a, b, (((1,), (0,)), ((), ())), preferred_element_type=F32)


def _kernel(n, groups, per, x_hbm, gain_ref, near_ref, far_ref, wq, wk, wv, wo, y_hbm,
            xb, ab, wbuf, wobuf, qt, kb, vt, kr, vr, cross, stat_s, stat_r, acc, ot, lse_s, obuf, rope,
            x_sem, w_sem, wo_sem, y_sem, ks_sem, kr_sem, vs_sem, vr_sem, cs_sem, cr_sem, ss_sem, sr_sem):
    own, d = xb.shape
    me = lax.axis_index("sp")
    partner = me + 1 - 2 * lax.rem(me, 2)
    other = n - 1 - me
    odd = lax.rem(me, 2) == 1
    low = me < n // 2
    scale = HEAD**-0.5
    e = scale * LOG2E
    steps = per + 2
    xrows = own // 4

    def x_copy(r):
        return pltpu.make_async_copy(x_hbm.at[pl.ds(r * xrows, xrows)], xb.at[pl.ds(r * xrows, xrows)], x_sem.at[r])

    def w_copies(g, slot):
        out = []
        for t in range(per):
            out.append(pltpu.make_async_copy(wq.at[:, pl.ds(pl.multiple_of((g * per + t) * HEAD, HEAD), HEAD)], wbuf.at[slot, t], w_sem.at[slot, t]))
        out.append(pltpu.make_async_copy(wk.at[:, pl.ds(pl.multiple_of(g * HEAD, HEAD), HEAD)], wbuf.at[slot, per], w_sem.at[slot, per]))
        out.append(pltpu.make_async_copy(wv.at[:, pl.ds(pl.multiple_of(g * HEAD, HEAD), HEAD)], wbuf.at[slot, per + 1], w_sem.at[slot, per + 1]))
        return out

    def wo_copy(g, slot):
        return pltpu.make_async_copy(wo.at[pl.ds(pl.multiple_of(g * per * HEAD, HEAD), per * HEAD), :], wobuf.at[slot], wo_sem.at[slot])

    def remote(src, dst, s, r, to):
        return pltpu.make_async_remote_copy(src_ref=src, dst_ref=dst, send_sem=s, recv_sem=r, device_id={"sp": to}, device_id_type=MESH)

    def k_move(g):
        return remote(kb.at[g], kr.at[g], ks_sem.at[g], kr_sem.at[g], partner)

    def v_move(g):
        return remote(vt.at[g], vr.at[g], vs_sem.at[g], vr_sem.at[g], partner)

    def q_move(g, h):
        return remote(qt.at[g, h], cross.at[g, h], cs_sem.at[g, h], cr_sem.at[g, h], other)

    def o_move(g, h):
        return remote(cross.at[g, h], cross.at[g, h], cs_sem.at[g, h], cr_sem.at[g, h], other)

    def s_move(g):
        return remote(stat_s.at[g], stat_r.at[g], ss_sem.at[g], sr_sem.at[g], other)

    for r in range(4):
        x_copy(r).start()
    for g in range(2):
        for c in w_copies(g, g):
            c.start()
        wo_copy(g, g).start()

    barrier = pltpu.get_barrier_semaphore()
    for to in (partner, other):
        pl.semaphore_signal(barrier, inc=1, device_id={"sp": to}, device_id_type=MESH)

    ca, sa = near_ref[0], near_ref[1]
    cf, sf = far_ref[0, pl.ds(me, 1), :], far_ref[1, pl.ds(me, 1), :]
    rope[0] = ca * cf - sa * sf
    rope[1] = sa * cf + ca * sf

    gain = gain_ref[...].astype(F32)
    nr = 64
    for r in range(4):
        x_copy(r).wait()

        def norm(j, _):
            rows = pl.ds(pl.multiple_of(r * xrows + j * nr, nr), nr)
            wide = xb[rows, :].astype(F32)
            inv = lax.rsqrt(jnp.mean(wide * wide, -1, keepdims=True) + 1e-6)
            ab[rows, :] = (wide * inv * gain).astype(BF16)
            return 0

        lax.fori_loop(0, xrows // nr, norm, 0)

    pl.semaphore_wait(barrier, 2)

    def turn(t):
        t = t.astype(BF16).astype(F32)
        half = HEAD // 2
        a, b = t[:, :half], t[:, half:]
        cos, sin = rope[0], rope[1]
        return jnp.concatenate([a * cos - b * sin, b * cos + a * sin], -1).astype(BF16)

    def project(g):
        slot = lax.rem(g, 2)
        copies = w_copies(g, slot)
        copies[per].wait()
        kb[g] = turn(_dot(ab[...], wbuf[slot, per]))

        @pl.when(me != n - 1)
        def _():
            k_move(g).start()

        copies[per + 1].wait()
        vt[g] = _dot(ab[...], wbuf[slot, per + 1]).astype(BF16).T

        @pl.when(me != n - 1)
        def _():
            v_move(g).start()

        for t in range(per):
            copies[t].wait()
            qt[g, t] = turn(_dot(ab[...], wbuf[slot, t])).T

            @pl.when(jnp.logical_not(low))
            def _():
                q_move(g, t).start()

        @pl.when(g + 2 < groups)
        def _():
            for c in w_copies(g + 2, slot):
                c.start()

    def parts(q, blocks):
        scores = []
        for k, _, masked in blocks:
            s = _dot(k, q)
            if masked:
                s = jnp.where(lax.broadcasted_iota(jnp.int32, s.shape, 0) <= lax.broadcasted_iota(jnp.int32, s.shape, 1), s, HIDDEN)
            scores.append(s)
        top = functools.reduce(jnp.maximum, [s.max(axis=0, keepdims=True) for s in scores])
        total, out = None, None
        for s, (_, v, _) in zip(scores, blocks):
            p = jnp.exp2((s - top) * e)
            add = p.sum(axis=0, keepdims=True)
            mix = _dot(v, p.astype(BF16))
            total, out = (add, mix) if total is None else (total + add, out + mix)
        return out * (1 / total), top * scale + jnp.log(total)

    def far_part(g):
        @pl.when(low)
        def _():
            k_move(g).wait_recv()
            v_move(g).wait_recv()
            for h in range(per):
                q_move(g, h).wait_recv()
                o, lse = parts(cross[g, h], [(kb[g], vt[g], False), (kr[g], vr[g], False)])
                cross[g, h] = o.astype(BF16)
                stat_s[g, h : h + 1, :] = lse
                o_move(g, h).start()
            s_move(g).start()

    def near_part(g):
        @pl.when(jnp.logical_not(odd))
        def _():
            for h in range(per):
                o, lse = parts(qt[g, h], [(kb[g], vt[g], True)])
                ot[h] = o
                lse_s[h : h + 1, :] = lse

        @pl.when(odd)
        def _():
            @pl.when(jnp.logical_not(low))
            def _():
                k_move(g).wait_recv()
                v_move(g).wait_recv()

            for h in range(per):
                o, lse = parts(qt[g, h], [(kb[g], vt[g], True), (kr[g], vr[g], False)])
                ot[h] = o
                lse_s[h : h + 1, :] = lse

        @pl.when(low)
        def _():
            for h in range(per):
                obuf[:, h * HEAD : (h + 1) * HEAD] = ot[h].astype(BF16).T

        @pl.when(jnp.logical_not(low))
        def _():
            s_move(g).wait_recv()
            for h in range(per):
                o_move(g, h).wait_recv()
                mine, theirs = lse_s[h : h + 1, :], stat_r[g, h : h + 1, :]
                top = jnp.maximum(mine, theirs)
                wm, wt = jnp.exp(mine - top), jnp.exp(theirs - top)
                inv = 1 / (wm + wt)
                o = ot[h] * (wm * inv) + cross[g, h].astype(F32) * (wt * inv)
                obuf[:, h * HEAD : (h + 1) * HEAD] = o.astype(BF16).T

    cols = 256

    def y_copy(j):
        at = pl.ds(pl.multiple_of(j * cols, cols), cols)
        return pltpu.make_async_copy(ab.at[:, at], y_hbm.at[:, at], y_sem)

    def out_part(g):
        slot = lax.rem(g, 2)
        wo_copy(g, slot).wait()

        def tile(j, _):
            at = pl.ds(pl.multiple_of(j * cols, cols), cols)
            add = _dot(obuf[...], wobuf[slot, :, at])

            @pl.when(g == 0)
            def _():
                acc[:, at] = xb[:, at].astype(F32) + add

            @pl.when(g > 0)
            def _():
                acc[:, at] += add

            return 0

        lax.fori_loop(0, d // cols, tile, 0)

        @pl.when(g + 2 < groups)
        def _():
            wo_copy(g + 2, slot).start()

    def step(i, _):
        @pl.when(i >= LEAD)
        def _():
            far_part(i - LEAD)

        @pl.when(i < groups)
        def _():
            project(i)

        @pl.when(i >= LEAD)
        def _():
            near_part(i - LEAD)
            out_part(i - LEAD)

        return 0

    lax.fori_loop(0, groups + LEAD, step, 0)

    def finish(j, _):
        at = pl.ds(pl.multiple_of(j * cols, cols), cols)
        ab[:, at] = acc[:, at].astype(BF16)
        return 0

    lax.fori_loop(0, d // cols, finish, 0)
    whole = pltpu.make_async_copy(ab, y_hbm, y_sem)
    whole.start()

    def drain(g, _):
        @pl.when(me != n - 1)
        def _():
            k_move(g).wait_send()
            v_move(g).wait_send()

        for h in range(per):
            q_move(g, h).wait_send()

        @pl.when(low)
        def _():
            s_move(g).wait_send()

        return 0

    lax.fori_loop(0, groups, drain, 0)
    whole.wait()


def _tables(n, own, half):
    rate = float(THETA) ** (-np.arange(half, dtype=np.float64) / half)
    near = np.arange(own, dtype=np.float64)[:, None] * rate
    far = (np.arange(n, dtype=np.float64) * own)[:, None] * rate
    return [np.stack([np.cos(t), np.sin(t)]).astype(np.float32) for t in (near, far)]


def solution(mesh):
    n = mesh.shape["sp"]

    def step(x, gain, wq, wk, wv, wo):
        own, d = x.shape
        groups = wk.shape[1] // HEAD
        per = wq.shape[1] // wk.shape[1]
        near, far = _tables(n, own, HEAD // 2)
        anyspace = pl.BlockSpec(memory_space=pl.ANY)
        vmem = pl.BlockSpec(memory_space=pltpu.VMEM)
        dma = pltpu.SemaphoreType.DMA
        return pl.pallas_call(
            functools.partial(_kernel, n, groups, per),
            out_shape=jax.ShapeDtypeStruct((own, d), BF16),
            in_specs=[anyspace, vmem, vmem, vmem, anyspace, anyspace, anyspace, anyspace],
            out_specs=anyspace,
            scratch_shapes=[
                pltpu.VMEM((own, d), BF16),
                pltpu.VMEM((own, d), BF16),
                pltpu.VMEM((2, per + 2, d, HEAD), BF16),
                pltpu.VMEM((2, per * HEAD, d), BF16),
                pltpu.VMEM((groups, per, HEAD, own), BF16),
                pltpu.VMEM((groups, own, HEAD), BF16),
                pltpu.VMEM((groups, HEAD, own), BF16),
                pltpu.VMEM((groups, own, HEAD), BF16),
                pltpu.VMEM((groups, HEAD, own), BF16),
                pltpu.VMEM((groups, per, HEAD, own), BF16),
                pltpu.VMEM((groups, 8, own), F32),
                pltpu.VMEM((groups, 8, own), F32),
                pltpu.VMEM((own, d), F32),
                pltpu.VMEM((per, HEAD, own), F32),
                pltpu.VMEM((8, own), F32),
                pltpu.VMEM((own, per * HEAD), BF16),
                pltpu.VMEM((2, own, HEAD // 2), F32),
                dma((4,)), dma((2, per + 2)), dma((2,)), dma(()),
                dma((groups,)), dma((groups,)), dma((groups,)), dma((groups,)),
                dma((groups, per)), dma((groups, per)), dma((groups,)), dma((groups,)),
            ],
            compiler_params=pltpu.CompilerParams(collective_id=0, has_side_effects=True, vmem_limit_bytes=67043328),
            cost_estimate=pl.CostEstimate(flops=2 * own * d * HEAD * groups * (2 * per + 2), transcendentals=0,
                                          bytes_accessed=2 * d * HEAD * groups * (2 * per + 2)),
        )(x, gain.reshape(1, d), near, far, wq, wk, wv, wo)

    tokens, whole = P(("dp", "sp"), None), P(None, None)
    return jax.shard_map(
        step,
        mesh=mesh,
        in_specs=(tokens, P(None), whole, whole, whole, whole),
        out_specs=tokens,
        check_vma=False,
    )
```

```python
import functools

import jax
import jax.numpy as jnp
import numpy as np
from jax import lax
from jax.experimental import pallas as pl
from jax.experimental.pallas import tpu as pltpu
from jax.sharding import PartitionSpec as P

HEAD = 256
THETA = 10000
HIDDEN = -2e30
LOG2E = 1.4426950408889634
MESH = pl.DeviceIdType.MESH
TILE = 256
LEAD = 3
F32, BF16 = jnp.float32, jnp.bfloat16


def _dot(a, b):
    return lax.dot_general(a, b, (((1,), (0,)), ((), ())), preferred_element_type=F32)


def _kernel(n, groups, per, x_hbm, gain_ref, near_ref, far_ref, wq, wk, wv, wo, y_hbm,
            xb, ab, wbuf, wobuf, qt, kb, vt, kr, vr, cross, stat_s, stat_r, acc, ot, lse_s, obuf, rope, s0, s1,
            x_sem, w_sem, wo_sem, y_sem, ks_sem, kr_sem, vs_sem, vr_sem, cs_sem, cr_sem, ss_sem, sr_sem):
    own, d = xb.shape
    me = lax.axis_index("sp")
    partner = me + 1 - 2 * lax.rem(me, 2)
    other = n - 1 - me
    odd = lax.rem(me, 2) == 1
    low = me < n // 2
    scale = HEAD**-0.5
    e = scale * LOG2E
    xrows = own // 4

    def x_copy(r):
        return pltpu.make_async_copy(x_hbm.at[pl.ds(r * xrows, xrows)], xb.at[pl.ds(r * xrows, xrows)], x_sem.at[r])

    def w_copies(g, slot):
        at = pl.ds(pl.multiple_of(g * HEAD, HEAD), HEAD)
        wide = pl.ds(pl.multiple_of(g * per * HEAD, per * HEAD), per * HEAD)
        return [
            pltpu.make_async_copy(wk.at[:, at], wbuf.at[slot, :, pl.ds(0, HEAD)], w_sem.at[slot, 0]),
            pltpu.make_async_copy(wv.at[:, at], wbuf.at[slot, :, pl.ds(HEAD, HEAD)], w_sem.at[slot, 1]),
            pltpu.make_async_copy(wq.at[:, wide], wbuf.at[slot, :, pl.ds(2 * HEAD, per * HEAD)], w_sem.at[slot, 2]),
        ]

    def wo_copy(g, slot):
        return pltpu.make_async_copy(wo.at[pl.ds(pl.multiple_of(g * per * HEAD, HEAD), per * HEAD), :], wobuf.at[slot], wo_sem.at[slot])

    def remote(src, dst, s, r, to):
        return pltpu.make_async_remote_copy(src_ref=src, dst_ref=dst, send_sem=s, recv_sem=r, device_id={"sp": to}, device_id_type=MESH)

    def k_move(g):
        return remote(kb.at[g], kr.at[g], ks_sem.at[g], kr_sem.at[g], partner)

    def v_move(g):
        return remote(vt.at[g], vr.at[g], vs_sem.at[g], vr_sem.at[g], partner)

    def q_move(g, h):
        return remote(qt.at[g, h], cross.at[g, h], cs_sem.at[g, h], cr_sem.at[g, h], other)

    def o_move(g, h):
        return remote(cross.at[g, h], cross.at[g, h], cs_sem.at[g, h], cr_sem.at[g, h], other)

    def s_move(g):
        return remote(stat_s.at[g], stat_r.at[g], ss_sem.at[g], sr_sem.at[g], other)

    for r in range(4):
        x_copy(r).start()
    for g in range(2):
        for c in w_copies(g, g):
            c.start()
        wo_copy(g, g).start()

    barrier = pltpu.get_barrier_semaphore()
    for to in (partner, other):
        pl.semaphore_signal(barrier, inc=1, device_id={"sp": to}, device_id_type=MESH)

    ca, sa = near_ref[0], near_ref[1]
    cf, sf = far_ref[0, pl.ds(me, 1), :], far_ref[1, pl.ds(me, 1), :]
    rope[0] = ca * cf - sa * sf
    rope[1] = sa * cf + ca * sf

    gain = gain_ref[...].astype(F32).reshape(1, d)
    nr = 64
    for r in range(4):
        x_copy(r).wait()

        def norm(j, _):
            rows = pl.ds(pl.multiple_of(r * xrows + j * nr, nr), nr)
            wide = xb[rows, :].astype(F32)
            inv = lax.rsqrt(jnp.mean(wide * wide, -1, keepdims=True) + 1e-6)
            ab[rows, :] = (wide * inv * gain).astype(BF16)
            return 0

        lax.fori_loop(0, xrows // nr, norm, 0)

    pl.semaphore_wait(barrier, 2)

    def turn(t):
        t = t.astype(BF16).astype(F32)
        half = HEAD // 2
        a, b = t[:, :half], t[:, half:]
        cos, sin = rope[0], rope[1]
        return jnp.concatenate([a * cos - b * sin, b * cos + a * sin], -1).astype(BF16)

    def project(g):
        slot = lax.rem(g, 2)
        copies = w_copies(g, slot)
        copies[0].wait()
        copies[1].wait()
        kv = _dot(ab[...], wbuf[slot, :, : 2 * HEAD])
        kb[g] = turn(kv[:, :HEAD])
        vt[g] = kv[:, HEAD:].astype(BF16).T
        k_move(g).start()
        v_move(g).start()
        copies[2].wait()
        q = _dot(ab[...], wbuf[slot, :, 2 * HEAD :])
        for t in range(per):
            qt[g, t] = turn(q[:, t * HEAD : (t + 1) * HEAD]).T

        @pl.when(jnp.logical_not(low))
        def _():
            for t in range(per):
                q_move(g, t).start()

        @pl.when(g + 2 < groups)
        def _():
            for c in w_copies(g + 2, slot):
                c.start()

    def attend(units):
        def scores(unit, buf):
            q, blocks, _ = unit
            top, row = None, 0
            for k, _, masked in blocks:
                t = _dot(k(), q())
                rows = t.shape[0]
                if masked:
                    seen = lax.broadcasted_iota(jnp.int32, t.shape, 0) <= lax.broadcasted_iota(jnp.int32, t.shape, 1)
                    t = jnp.where(seen, t, HIDDEN)
                buf[row : row + rows, :] = t
                most = t.reshape(rows // 8, 8, TILE).max(axis=0)
                top = most if top is None else jnp.maximum(top, most)
                row += rows
            return top.max(axis=0, keepdims=True)

        def mix(unit, buf, top):
            _, blocks, done = unit
            out, total, row = None, None, 0
            for _, v, _ in blocks:
                vals = v()
                for c in range(0, vals.shape[1], TILE):
                    p = jnp.exp2((buf[row : row + TILE, :] - top) * e)
                    add = p.reshape(TILE // 8, 8, TILE).sum(axis=0)
                    part = _dot(vals[:, c : c + TILE], p.astype(BF16))
                    total, out = (add, part) if out is None else (total + add, out + part)
                    row += TILE
            total = total.sum(axis=0, keepdims=True)
            done(out * (1 / total), top * scale + jnp.log(total))

        bufs = (s0, s1)
        top = scores(units[0], bufs[0])
        for u, unit in enumerate(units):
            after = scores(units[u + 1], bufs[(u + 1) % 2]) if u + 1 < len(units) else None
            mix(unit, bufs[u % 2], top)
            top = after

    halves = range(0, own, TILE)

    def far_units(g):
        def make(h, at):
            def done(o, lse):
                cross[g, h, :, at : at + TILE] = o.astype(BF16)
                stat_s[g, h : h + 1, at : at + TILE] = lse
                if at + TILE == own:
                    o_move(g, h).start()
                    if h + 1 == per:
                        s_move(g).start()

            blocks = [(lambda: kb[g], lambda: vt[g], False), (lambda: kr[g], lambda: vr[g], False)]
            return lambda: cross[g, h, :, at : at + TILE], blocks, done

        return [make(h, at) for h in range(per) for at in halves]

    def near_units(g, with_partner, keep):
        def make(h, at):
            def done(o, lse):
                if keep:
                    ot[h, :, at : at + TILE] = o
                    lse_s[h : h + 1, at : at + TILE] = lse
                else:
                    obuf[at : at + TILE, h * HEAD : (h + 1) * HEAD] = o.astype(BF16).T

            blocks = [(lambda: kb[g, at : at + TILE, :], lambda: vt[g, :, at : at + TILE], True)]
            if at:
                blocks.append((lambda: kb[g, :at, :], lambda: vt[g, :, :at], False))
            if with_partner:
                blocks.append((lambda: kr[g], lambda: vr[g], False))
            return lambda: qt[g, h, :, at : at + TILE], blocks, done

        return [make(h, at) for h in range(per) for at in halves]

    def far_part(g):
        @pl.when(low)
        def _():
            k_move(g).wait_recv()
            v_move(g).wait_recv()
            for h in range(per):
                q_move(g, h).wait_recv()
            attend(far_units(g))

    def near_part(g):
        for right in (False, True):

            @pl.when(low & (odd == right))
            def _():
                attend(near_units(g, right, False))

        @pl.when(jnp.logical_not(low))
        def _():
            k_move(g).wait_recv()
            v_move(g).wait_recv()
            for right in (False, True):

                @pl.when(odd == right)
                def _():
                    attend(near_units(g, right, True))

            s_move(g).wait_recv()
            for h in range(per):
                o_move(g, h).wait_recv()
                mine, theirs = lse_s[h : h + 1, :], stat_r[g, h : h + 1, :]
                top = jnp.maximum(mine, theirs)
                wm, wt = jnp.exp(mine - top), jnp.exp(theirs - top)
                inv = 1 / (wm + wt)
                o = ot[h] * (wm * inv) + cross[g, h].astype(F32) * (wt * inv)
                obuf[:, h * HEAD : (h + 1) * HEAD] = o.astype(BF16).T

    cols = 2 * HEAD

    def y_copy(at):
        return pltpu.make_async_copy(ab.at[:, pl.ds(at, cols)], y_hbm.at[:, pl.ds(at, cols)], y_sem.at[at // cols])

    def out_part(g):
        slot = lax.rem(g, 2)
        wo_copy(g, slot).wait()

        @pl.when(g < groups - 1)
        def _():
            for at in range(0, d, cols):
                add = _dot(obuf[...], wobuf[slot, :, at : at + cols])
                acc[:, at : at + cols] = jnp.where(g > 0, acc[:, at : at + cols], 0.0) + add

        @pl.when(g == groups - 1)
        def _():
            for at in range(0, d, cols):
                add = _dot(obuf[...], wobuf[slot, :, at : at + cols])
                ab[:, at : at + cols] = (xb[:, at : at + cols].astype(F32) + (acc[:, at : at + cols] + add)).astype(BF16)
                y_copy(at).start()

        @pl.when(g + 2 < groups)
        def _():
            wo_copy(g + 2, slot).start()

    def step(i, _):
        @pl.when(i >= LEAD)
        def _():
            far_part(i - LEAD)

        @pl.when(i < groups)
        def _():
            project(i)

        @pl.when(i >= LEAD)
        def _():
            near_part(i - LEAD)
            out_part(i - LEAD)

        return 0

    lax.fori_loop(0, groups + LEAD, step, 0)

    def drain(g, _):
        k_move(g).wait_send()
        v_move(g).wait_send()

        for h in range(per):
            q_move(g, h).wait_send()

        @pl.when(low)
        def _():
            s_move(g).wait_send()

        return 0

    lax.fori_loop(0, groups, drain, 0)
    for at in range(0, d, cols):
        y_copy(at).wait()


def _tables(n, own, half):
    rate = float(THETA) ** (-np.arange(half, dtype=np.float64) / half)
    near = np.arange(own, dtype=np.float64)[:, None] * rate
    far = (np.arange(n, dtype=np.float64) * own)[:, None] * rate
    return [np.stack([np.cos(t), np.sin(t)]).astype(np.float32) for t in (near, far)]


def solution(mesh):
    n = mesh.shape["sp"]

    def step(x, gain, wq, wk, wv, wo):
        own, d = x.shape
        groups = wk.shape[1] // HEAD
        per = wq.shape[1] // wk.shape[1]
        near, far = _tables(n, own, HEAD // 2)
        anyspace = pl.BlockSpec(memory_space=pl.ANY)
        vmem = pl.BlockSpec(memory_space=pltpu.VMEM)
        dma = pltpu.SemaphoreType.DMA
        return pl.pallas_call(
            functools.partial(_kernel, n, groups, per),
            out_shape=jax.ShapeDtypeStruct((own, d), BF16),
            in_specs=[anyspace, vmem, vmem, vmem, anyspace, anyspace, anyspace, anyspace],
            out_specs=anyspace,
            scratch_shapes=[
                pltpu.VMEM((own, d), BF16),
                pltpu.VMEM((own, d), BF16),
                pltpu.VMEM((2, d, (per + 2) * HEAD), BF16),
                pltpu.VMEM((2, per * HEAD, d), BF16),
                pltpu.VMEM((groups, per, HEAD, own), BF16),
                pltpu.VMEM((groups, own, HEAD), BF16),
                pltpu.VMEM((groups, HEAD, own), BF16),
                pltpu.VMEM((groups, own, HEAD), BF16),
                pltpu.VMEM((groups, HEAD, own), BF16),
                pltpu.VMEM((groups, per, HEAD, own), BF16),
                pltpu.VMEM((groups, 8, own), F32),
                pltpu.VMEM((groups, 8, own), F32),
                pltpu.VMEM((own, d), F32),
                pltpu.VMEM((per, HEAD, own), F32),
                pltpu.VMEM((8, own), F32),
                pltpu.VMEM((own, per * HEAD), BF16),
                pltpu.VMEM((2, own, HEAD // 2), F32),
                pltpu.VMEM((2 * own, TILE), F32),
                pltpu.VMEM((2 * own, TILE), F32),
                dma((4,)), dma((2, 3)), dma((2,)), dma((d // (2 * HEAD),)),
                dma((groups,)), dma((groups,)), dma((groups,)), dma((groups,)),
                dma((groups, per)), dma((groups, per)), dma((groups,)), dma((groups,)),
            ],
            compiler_params=pltpu.CompilerParams(collective_id=0, has_side_effects=True, vmem_limit_bytes=67043328),
            cost_estimate=pl.CostEstimate(flops=2 * own * d * HEAD * groups * (2 * per + 2), transcendentals=0,
                                          bytes_accessed=2 * d * HEAD * groups * (2 * per + 2)),
        )(x, gain, near, far, wq, wk, wv, wo)

    tokens, whole = P(("dp", "sp"), None), P(None, None)
    return jax.shard_map(
        step,
        mesh=mesh,
        in_specs=(tokens, P(None), whole, whole, whole, whole),
        out_specs=tokens,
        check_vma=False,
    )
```

```python
import functools

import jax
import jax.numpy as jnp
import numpy as np
from jax import lax
from jax.experimental import pallas as pl
from jax.experimental.pallas import tpu as pltpu
from jax.sharding import PartitionSpec as P

HEAD = 256
THETA = 10000
HIDDEN = -2e30
LOG2E = 1.4426950408889634
MESH = pl.DeviceIdType.MESH
TILE = 256
LANES = 128
DIRECT = 1
LATE = 4
LEAD = 3
F32, BF16 = jnp.float32, jnp.bfloat16


def _dot(a, b):
    return lax.dot_general(a, b, (((1,), (0,)), ((), ())), preferred_element_type=F32)


def _kernel(n, groups, per, x_hbm, gain_ref, near_ref, far_ref, wq, wk, wv, wo, y_hbm,
            xb, ab, wbuf, wobuf, qt, kb, vt, kr, vr, kd, vd, cross, stat_s, stat_r, acc, ot, lse_s, obuf, rope, s0, s1,
            x_sem, t_sem, w_sem, wo_sem, y_sem, ks_sem, kr_sem, vs_sem, vr_sem, kds_sem, kdr_sem, vds_sem, vdr_sem,
            cs_sem, cr_sem, ss_sem, sr_sem):
    own, d = xb.shape
    me = lax.axis_index("sp")
    partner = me + 1 - 2 * lax.rem(me, 2)
    other = n - 1 - me
    odd = lax.rem(me, 2) == 1
    low = me < n // 2
    high = jnp.logical_not(low)
    last = groups - 1

    def order(j):
        at = jnp.where(low, last, last - 2)
        return jnp.where(j == at, DIRECT, jnp.where((j >= DIRECT) & (j < at), j + 1, j))

    scale = HEAD**-0.5
    e = scale * LOG2E
    xrows = own // 4

    def x_copy(r):
        return pltpu.make_async_copy(x_hbm.at[pl.ds(r * xrows, xrows)], xb.at[pl.ds(r * xrows, xrows)], x_sem.at[r])

    def w_copies(g, slot):
        at = pl.ds(pl.multiple_of(g * HEAD, HEAD), HEAD)
        wide = pl.ds(pl.multiple_of(g * per * HEAD, per * HEAD), per * HEAD)
        return [
            pltpu.make_async_copy(wk.at[:, at], wbuf.at[slot, :, pl.ds(0, HEAD)], w_sem.at[slot, 0]),
            pltpu.make_async_copy(wv.at[:, at], wbuf.at[slot, :, pl.ds(HEAD, HEAD)], w_sem.at[slot, 1]),
            pltpu.make_async_copy(wq.at[:, wide], wbuf.at[slot, :, pl.ds(2 * HEAD, per * HEAD)], w_sem.at[slot, 2]),
        ]

    def wo_copy(g, slot):
        return pltpu.make_async_copy(wo.at[pl.ds(pl.multiple_of(g * per * HEAD, HEAD), per * HEAD), :], wobuf.at[slot], wo_sem.at[slot])

    def remote(src, dst, s, r, to):
        return pltpu.make_async_remote_copy(src_ref=src, dst_ref=dst, send_sem=s, recv_sem=r, device_id={"sp": to}, device_id_type=MESH)

    def k_move(g):
        return remote(kb.at[g], kr.at[g], ks_sem.at[g], kr_sem.at[g], partner)

    def v_move(g):
        return remote(vt.at[g], vr.at[g], vs_sem.at[g], vr_sem.at[g], partner)

    def q_move(g, h):
        return remote(qt.at[g, h], cross.at[g, h], cs_sem.at[g, h], cr_sem.at[g, h], other)

    def o_move(g, h):
        return remote(cross.at[g, h], cross.at[g, h], cs_sem.at[g, h], cr_sem.at[g, h], other)

    def s_move(g, h):
        return remote(stat_s.at[g, h], stat_r.at[g, h], ss_sem.at[g, h], sr_sem.at[g, h], other)

    def kd_move(slot, src, to):
        return remote(src, kd.at[slot], kds_sem.at[slot], kdr_sem.at[slot], to)

    def vd_move(slot, src, to):
        return remote(src, vd.at[slot], vds_sem.at[slot], vdr_sem.at[slot], to)

    def is_device(i):
        return me == i

    for r in range(4):
        x_copy(r).start()
    table = pltpu.make_async_copy(near_ref, rope, t_sem)
    table.start()
    first = w_copies(0, 0)
    first[0].start()
    first[1].start()

    barrier = pltpu.get_barrier_semaphore()
    for to in (partner, other):
        pl.semaphore_signal(barrier, inc=1, device_id={"sp": to}, device_id_type=MESH)

    gain = gain_ref[...].astype(F32).reshape(1, d)
    nr = 64
    for r in range(4):
        x_copy(r).wait()
        if r == 3:
            first[2].start()
            for c in w_copies(1, 1):
                c.start()
            for j in range(2):
                wo_copy(order(j), j).start()

        def norm(j, _):
            rows = pl.ds(pl.multiple_of(r * xrows + j * nr, nr), nr)
            wide = xb[rows, :].astype(F32)
            inv = lax.rsqrt(jnp.mean(wide * wide, -1, keepdims=True) + 1e-6)
            ab[rows, :] = (wide * inv * gain).astype(BF16)
            return 0

        lax.fori_loop(0, xrows // nr, norm, 0)

    table.wait()
    ca, sa = rope[0], rope[1]
    cf, sf = far_ref[0, pl.ds(me, 1), :], far_ref[1, pl.ds(me, 1), :]
    rope[0] = ca * cf - sa * sf
    rope[1] = sa * cf + ca * sf
    pl.semaphore_wait(barrier, 2)

    def turn(t):
        t = t.astype(BF16).astype(F32)
        half = HEAD // 2
        a, b = t[:, :half], t[:, half:]
        cos, sin = rope[0], rope[1]
        return jnp.concatenate([a * cos - b * sin, b * cos + a * sin], -1).astype(BF16)

    def project(g):
        slot = lax.rem(g, 2)
        copies = w_copies(g, slot)
        copies[0].wait()
        copies[1].wait()
        kv = _dot(ab[...], wbuf[slot, :, : 2 * HEAD])
        kb[g] = turn(kv[:, :HEAD])
        vt[g] = kv[:, HEAD:].astype(BF16).T

        @pl.when((me != n - 1) & (g != DIRECT) | is_device(n - 2))
        def _():
            k_move(g).start()
            v_move(g).start()

        @pl.when(low & (g == DIRECT))
        def _():
            kd_move(me, kb.at[g], other).start()
            vd_move(me, vt.at[g], other).start()

        @pl.when(is_device(1) & (g == LATE))
        def _():
            v_move(DIRECT).start()

        @pl.when(is_device(0) & (g == last))
        def _():
            k_move(DIRECT).start()
            v_move(DIRECT).start()

        copies[2].wait()
        q = _dot(ab[...], wbuf[slot, :, 2 * HEAD :])
        for t in range(per):
            qt[g, t] = turn(q[:, t * HEAD : (t + 1) * HEAD]).T

        @pl.when(high & (g != DIRECT))
        def _():
            for t in range(per):
                q_move(g, t).start()

        @pl.when(g + 2 < groups)
        def _():
            for c in w_copies(g + 2, slot):
                c.start()

    def attend(units):
        def scores(unit, buf):
            q, blocks, _ = unit
            top, row = None, 0
            for k, _, masked in blocks:
                t = _dot(k(), q())
                rows = t.shape[0]
                if masked:
                    seen = lax.broadcasted_iota(jnp.int32, t.shape, 0) <= lax.broadcasted_iota(jnp.int32, t.shape, 1)
                    t = jnp.where(seen, t, HIDDEN)
                buf[row : row + rows, :] = t
                most = t.reshape(rows // 8, 8, TILE).max(axis=0)
                top = most if top is None else jnp.maximum(top, most)
                row += rows
            return top.max(axis=0, keepdims=True)

        def mix(unit, buf, top):
            _, blocks, done = unit
            out, total, row = None, None, 0
            for _, v, _ in blocks:
                vals = v()
                for c in range(0, vals.shape[1], TILE):
                    p = jnp.exp2((buf[row : row + TILE, :] - top) * e)
                    add = p.reshape(TILE // 8, 8, TILE).sum(axis=0)
                    part = _dot(vals[:, c : c + TILE], p.astype(BF16))
                    total, out = (add, part) if out is None else (total + add, out + part)
                    row += TILE
            total = total.sum(axis=0, keepdims=True)
            done(out * (1 / total), top * scale + jnp.log(total))

        bufs = (s0, s1)
        top = scores(units[0], bufs[0])
        for u, unit in enumerate(units):
            after = scores(units[u + 1], bufs[(u + 1) % 2]) if u + 1 < len(units) else None
            mix(unit, bufs[u % 2], top)
            top = after

    halves = range(0, own, TILE)

    def far_units(g):
        def make(h, at):
            def done(o, lse):
                cross[g, h, :, at : at + TILE] = o.astype(BF16)
                for c in range(0, TILE, LANES):
                    stat_s[g, h, (at + c) // LANES : (at + c) // LANES + 1, :] = lse[:, c : c + LANES]
                if at + TILE == own:
                    s_move(g, h).start()
                    o_move(g, h).start()

            blocks = [(lambda: kb[g], lambda: vt[g], False), (lambda: kr[g], lambda: vr[g], False)]
            return lambda: cross[g, h, :, at : at + TILE], blocks, done

        return [make(h, at) for h in range(per) for at in halves]

    def near_units(g, with_partner, with_direct, keep):
        def make(h, at):
            def done(o, lse):
                if keep:
                    ot[h, :, at : at + TILE] = o
                    lse_s[h : h + 1, at : at + TILE] = lse
                else:
                    obuf[at : at + TILE, h * HEAD : (h + 1) * HEAD] = o.astype(BF16).T

            blocks = [(lambda: kb[g, at : at + TILE, :], lambda: vt[g, :, at : at + TILE], True)]
            if at:
                blocks.append((lambda: kb[g, :at, :], lambda: vt[g, :, :at], False))
            if with_partner:
                blocks.append((lambda: kr[g], lambda: vr[g], False))
            if with_direct:
                blocks += [(lambda i=i: kd[i], lambda i=i: vd[i], False) for i in range(2)]
            return lambda: qt[g, h, :, at : at + TILE], blocks, done

        return [make(h, at) for h in range(per) for at in halves]

    def far_part(g):
        @pl.when(low & (g != DIRECT))
        def _():
            k_move(g).wait_recv()
            v_move(g).wait_recv()
            for h in range(per):
                q_move(g, h).wait_recv()
            attend(far_units(g))

    def forward():
        @pl.when(is_device(n - 2))
        def _():
            kd_move(1, kb.at[DIRECT], other).wait_recv()
            kd_move(1, kd.at[1], partner).start()

        @pl.when(is_device(n - 1))
        def _():
            kd_move(0, kb.at[DIRECT], other).wait_recv()
            vd_move(0, vt.at[DIRECT], other).wait_recv()
            kd_move(0, kd.at[0], partner).start()
            vd_move(0, vd.at[0], partner).start()

    def forward_late():
        @pl.when(is_device(0))
        def _():
            v_move(DIRECT).wait_recv()
            vd_move(1, vr.at[DIRECT], other).start()

    def near_part(g):
        direct = g == DIRECT

        @pl.when(is_device(1) & direct)
        def _():
            k_move(g).wait_recv()
            v_move(g).wait_recv()

        for right in (False, True):

            @pl.when(low & (odd == right))
            def _():
                attend(near_units(g, right, False, False))

        @pl.when(is_device(n - 1))
        def _():
            k_move(g).wait_recv()
            v_move(g).wait_recv()

        for right in (False, True):

            @pl.when(high & (odd == right) & jnp.logical_not(direct))
            def _():
                attend(near_units(g, right, False, True))

            @pl.when(high & (odd == right) & direct)
            def _():
                if right:
                    kd_move(1, kd.at[1], partner).wait_recv()
                else:
                    kd_move(0, kd.at[0], partner).wait_recv()
                    vd_move(0, vd.at[0], partner).wait_recv()
                vd_move(1, vd.at[1], partner).wait_recv()
                attend(near_units(g, right, True, False))

    def merge(g, h):
        s_move(g, h).wait_recv()
        o_move(g, h).wait_recv()
        mine = lse_s[h : h + 1, :]
        theirs = jnp.concatenate([stat_r[g, h, c : c + 1, :] for c in range(own // LANES)], axis=1)
        top = jnp.maximum(mine, theirs)
        wm, wt = jnp.exp(mine - top), jnp.exp(theirs - top)
        inv = 1 / (wm + wt)
        o = ot[h] * (wm * inv) + cross[g, h].astype(F32) * (wt * inv)
        obuf[:, h * HEAD : (h + 1) * HEAD] = o.astype(BF16).T

    cols = 2 * HEAD

    def y_copy(at):
        return pltpu.make_async_copy(ab.at[:, pl.ds(at, cols)], y_hbm.at[:, pl.ds(at, cols)], y_sem.at[at // cols])

    def out_part(j, g):
        slot = lax.rem(j, 2)
        wo_copy(g, slot).wait()

        def gather(rows):
            for at in range(0, d, cols):
                add = _dot(obuf[:, rows], wobuf[slot, rows, at : at + cols])
                acc[:, at : at + cols] = jnp.where(j > 0, acc[:, at : at + cols], 0.0) + add

        def close(rows):
            for at in range(0, d, cols):
                add = _dot(obuf[:, rows], wobuf[slot, rows, at : at + cols])
                ab[:, at : at + cols] = (xb[:, at : at + cols].astype(F32) + (acc[:, at : at + cols] + add)).astype(BF16)
                y_copy(at).start()

        whole, early, late = slice(0, per * HEAD), slice(0, (per - 1) * HEAD), slice((per - 1) * HEAD, per * HEAD)

        @pl.when(high & (g != DIRECT) & (j < last))
        def _():
            for h in range(per):
                merge(g, h)

        @pl.when(j < last)
        def _():
            gather(whole)

        @pl.when(low & (j == last))
        def _():
            close(whole)

        @pl.when(high & (j == last))
        def _():
            for h in range(per - 1):
                merge(g, h)
            gather(early)
            merge(g, per - 1)
            close(late)

        @pl.when(j + 2 < groups)
        def _():
            wo_copy(order(j + 2), slot).start()

    def step(i, _):
        j = i - LEAD
        g = order(j)

        @pl.when(i >= LEAD)
        def _():
            far_part(g)

        @pl.when(i < groups)
        def _():
            project(i)

        @pl.when(i == LEAD)
        def _():
            forward()

        @pl.when(j == LATE)
        def _():
            forward_late()

        @pl.when(i >= LEAD)
        def _():
            near_part(g)
            out_part(j, g)

        return 0

    lax.fori_loop(0, groups + LEAD, step, 0)

    def drain(g, _):
        usual = g != DIRECT

        @pl.when((me != n - 1) & usual | is_device(n - 2) | is_device(0))
        def _():
            k_move(g).wait_send()

        @pl.when(me != n - 1)
        def _():
            v_move(g).wait_send()

        @pl.when(usual)
        def _():
            for h in range(per):
                q_move(g, h).wait_send()

        @pl.when(low & usual)
        def _():
            for h in range(per):
                s_move(g, h).wait_send()

        return 0

    lax.fori_loop(0, groups, drain, 0)

    @pl.when(low)
    def _():
        kd_move(me, kb.at[DIRECT], other).wait_send()
        vd_move(me, vt.at[DIRECT], other).wait_send()

    @pl.when(is_device(0))
    def _():
        vd_move(1, vr.at[DIRECT], other).wait_send()

    @pl.when(is_device(n - 2))
    def _():
        kd_move(1, kd.at[1], partner).wait_send()

    @pl.when(is_device(n - 1))
    def _():
        kd_move(0, kd.at[0], partner).wait_send()
        vd_move(0, vd.at[0], partner).wait_send()

    for at in range(0, d, cols):
        y_copy(at).wait()


def _tables(n, own, half):
    rate = float(THETA) ** (-np.arange(half, dtype=np.float64) / half)
    near = np.arange(own, dtype=np.float64)[:, None] * rate
    far = (np.arange(n, dtype=np.float64) * own)[:, None] * rate
    return [np.stack([np.cos(t), np.sin(t)]).astype(np.float32) for t in (near, far)]


def solution(mesh):
    n = mesh.shape["sp"]

    def step(x, gain, wq, wk, wv, wo):
        own, d = x.shape
        groups = wk.shape[1] // HEAD
        per = wq.shape[1] // wk.shape[1]
        near, far = _tables(n, own, HEAD // 2)
        anyspace = pl.BlockSpec(memory_space=pl.ANY)
        vmem = pl.BlockSpec(memory_space=pltpu.VMEM)
        dma = pltpu.SemaphoreType.DMA
        return pl.pallas_call(
            functools.partial(_kernel, n, groups, per),
            out_shape=jax.ShapeDtypeStruct((own, d), BF16),
            in_specs=[anyspace, vmem, anyspace, vmem, anyspace, anyspace, anyspace, anyspace],
            out_specs=anyspace,
            scratch_shapes=[
                pltpu.VMEM((own, d), BF16),
                pltpu.VMEM((own, d), BF16),
                pltpu.VMEM((2, d, (per + 2) * HEAD), BF16),
                pltpu.VMEM((2, per * HEAD, d), BF16),
                pltpu.VMEM((groups, per, HEAD, own), BF16),
                pltpu.VMEM((groups, own, HEAD), BF16),
                pltpu.VMEM((groups, HEAD, own), BF16),
                pltpu.VMEM((groups, own, HEAD), BF16),
                pltpu.VMEM((groups, HEAD, own), BF16),
                pltpu.VMEM((2, own, HEAD), BF16),
                pltpu.VMEM((2, HEAD, own), BF16),
                pltpu.VMEM((groups, per, HEAD, own), BF16),
                pltpu.VMEM((groups, per, 8, LANES), F32),
                pltpu.VMEM((groups, per, 8, LANES), F32),
                pltpu.VMEM((own, d), F32),
                pltpu.VMEM((per, HEAD, own), F32),
                pltpu.VMEM((8, own), F32),
                pltpu.VMEM((own, per * HEAD), BF16),
                pltpu.VMEM((2, own, HEAD // 2), F32),
                pltpu.VMEM((4 * own, TILE), F32),
                pltpu.VMEM((4 * own, TILE), F32),
                dma((4,)), dma(()), dma((2, 3)), dma((2,)), dma((d // (2 * HEAD),)),
                dma((groups,)), dma((groups,)), dma((groups,)), dma((groups,)),
                dma((2,)), dma((2,)), dma((2,)), dma((2,)),
                dma((groups, per)), dma((groups, per)), dma((groups, per)), dma((groups, per)),
            ],
            compiler_params=pltpu.CompilerParams(collective_id=0, has_side_effects=True, vmem_limit_bytes=67043328),
            cost_estimate=pl.CostEstimate(flops=2 * own * d * HEAD * groups * (2 * per + 2), transcendentals=0,
                                          bytes_accessed=2 * d * HEAD * groups * (2 * per + 2)),
        )(x, gain, near, far, wq, wk, wv, wo)

    tokens, whole = P(("dp", "sp"), None), P(None, None)
    return jax.shard_map(
        step,
        mesh=mesh,
        in_specs=(tokens, P(None), whole, whole, whole, whole),
        out_specs=tokens,
        check_vma=False,
    )
```

```python
import functools

import jax
import jax.numpy as jnp
import numpy as np
from jax import lax
from jax.experimental import pallas as pl
from jax.experimental.pallas import tpu as pltpu
from jax.sharding import PartitionSpec as P

HEAD = 256
THETA = 10000
HIDDEN = -2e30
LOG2E = 1.4426950408889634
MESH = pl.DeviceIdType.MESH
TILE = 256
LANES = 128
DIRECT = 1
LATE = 4
LEAD = 3
F32, BF16 = jnp.float32, jnp.bfloat16


def _dot(a, b):
    return lax.dot_general(a, b, (((1,), (0,)), ((), ())), preferred_element_type=F32)


def _kernel(n, groups, per, x_hbm, gain_ref, near_ref, far_ref, wq, wk, wv, wo, y_hbm,
            ab, wbuf, wobuf, qt, kb, vt, kr, vr, kd, vd, cross, stat_s, stat_r, acc, ot, lse_s, obuf, rope, s0, s1,
            x_sem, t_sem, w_sem, wo_sem, y_sem, ks_sem, kr_sem, vs_sem, vr_sem, kds_sem, kdr_sem, vds_sem, vdr_sem,
            cs_sem, cr_sem, ss_sem, sr_sem):
    own, d = ab.shape
    me = lax.axis_index("sp")
    partner = me + 1 - 2 * lax.rem(me, 2)
    other = n - 1 - me
    odd = lax.rem(me, 2) == 1
    low = me < n // 2
    high = jnp.logical_not(low)
    last = groups - 1

    def order(j):
        at = jnp.where(low, last, last - 2)
        return jnp.where(j == at, DIRECT, jnp.where((j >= DIRECT) & (j < at), j + 1, j))

    scale = HEAD**-0.5
    e = scale * LOG2E
    xrows = own // 4

    def x_copy(r):
        return pltpu.make_async_copy(x_hbm.at[pl.ds(r * xrows, xrows)], ab.at[pl.ds(r * xrows, xrows)], x_sem.at[r])

    def w_copy(g, slot, which):
        at = pl.ds(pl.multiple_of(g * HEAD, HEAD), HEAD)
        wide = pl.ds(pl.multiple_of(g * per * HEAD, per * HEAD), per * HEAD)
        src, into = [(wk.at[:, at], pl.ds(0, HEAD)), (wv.at[:, at], pl.ds(HEAD, HEAD)), (wq.at[:, wide], pl.ds(2 * HEAD, per * HEAD))][which]
        return pltpu.make_async_copy(src, wbuf.at[slot, :, into], w_sem.at[slot, which])

    def wo_copy(g, slot):
        return pltpu.make_async_copy(wo.at[pl.ds(pl.multiple_of(g * per * HEAD, HEAD), per * HEAD), :], wobuf.at[slot], wo_sem.at[slot])

    def remote(src, dst, s, r, to):
        return pltpu.make_async_remote_copy(src_ref=src, dst_ref=dst, send_sem=s, recv_sem=r, device_id={"sp": to}, device_id_type=MESH)

    def k_move(g):
        return remote(kb.at[g], kr.at[g], ks_sem.at[g], kr_sem.at[g], partner)

    def v_move(g):
        return remote(vt.at[g], vr.at[g], vs_sem.at[g], vr_sem.at[g], partner)

    def q_move(g, h):
        return remote(qt.at[g, h], cross.at[g, h], cs_sem.at[g, h], cr_sem.at[g, h], other)

    def o_move(g, h):
        return remote(cross.at[g, h], cross.at[g, h], cs_sem.at[g, h], cr_sem.at[g, h], other)

    def s_move(g, h):
        return remote(stat_s.at[g, h, pl.ds(0, own // LANES)], stat_r.at[g, h, pl.ds(0, own // LANES)], ss_sem.at[g, h], sr_sem.at[g, h], other)

    def kd_move(slot, src, to):
        return remote(src, kd.at[slot], kds_sem.at[slot], kdr_sem.at[slot], to)

    def vd_move(slot, src, to):
        return remote(src, vd.at[slot], vds_sem.at[slot], vdr_sem.at[slot], to)

    def is_device(i):
        return me == i

    for r in range(4):
        x_copy(r).start()
    table = pltpu.make_async_copy(near_ref, rope, t_sem)
    table.start()
    w_copy(0, 0, 0).start()
    w_copy(0, 0, 1).start()

    barrier = pltpu.get_barrier_semaphore()
    for to in (partner, other):
        pl.semaphore_signal(barrier, inc=1, device_id={"sp": to}, device_id_type=MESH)

    gain = gain_ref[...].astype(F32).reshape(1, d)
    nr = 64
    for r in range(4):
        x_copy(r).wait()
        if r == 3:
            for g, which in ((1, 0), (1, 1), (0, 2), (1, 2)):
                w_copy(g, g, which).start()

        def norm(j, _):
            rows = pl.ds(pl.multiple_of(r * xrows + j * nr, nr), nr)
            wide = ab[rows, :].astype(F32)
            inv = lax.rsqrt(jnp.mean(wide * wide, -1, keepdims=True) + 1e-6)
            ab[rows, :] = (wide * inv * gain).astype(BF16)
            return 0

        lax.fori_loop(0, xrows // nr, norm, 0)

    table.wait()
    ca, sa = rope[0], rope[1]
    cf, sf = far_ref[0, pl.ds(me, 1), :], far_ref[1, pl.ds(me, 1), :]
    rope[0] = ca * cf - sa * sf
    rope[1] = sa * cf + ca * sf

    def turn(t):
        t = t.astype(BF16).astype(F32)
        half = HEAD // 2
        a, b = t[:, :half], t[:, half:]
        cos, sin = rope[0], rope[1]
        return jnp.concatenate([a * cos - b * sin, b * cos + a * sin], -1).astype(BF16)

    def project_kv(g, entering):
        slot = lax.rem(g, 2)
        w_copy(g, slot, 0).wait()
        w_copy(g, slot, 1).wait()
        kv = _dot(ab[...], wbuf[slot, :, : 2 * HEAD])
        kb[g] = turn(kv[:, :HEAD])
        vt[g] = kv[:, HEAD:].astype(BF16).T

        if entering:

            @pl.when(g == 0)
            def _():
                pl.semaphore_wait(barrier, 2)

        @pl.when((me != n - 1) & (g != DIRECT) | is_device(n - 2))
        def _():
            k_move(g).start()
            v_move(g).start()

        @pl.when(low & (g == DIRECT))
        def _():
            kd_move(me, kb.at[g], other).start()
            vd_move(me, vt.at[g], other).start()

        @pl.when(is_device(1) & (g == LATE))
        def _():
            v_move(DIRECT).start()

        @pl.when(is_device(0) & (g == last))
        def _():
            k_move(DIRECT).start()
            v_move(DIRECT).start()

    def project_q(g):
        slot = lax.rem(g, 2)
        w_copy(g, slot, 2).wait()
        q = _dot(ab[...], wbuf[slot, :, 2 * HEAD :])
        for t in range(per):
            qt[g, t] = turn(q[:, t * HEAD : (t + 1) * HEAD]).T

        @pl.when(high & (g != DIRECT))
        def _():
            for t in range(per):
                q_move(g, t).start()

        @pl.when(g + 2 < groups)
        def _():
            for which in range(3):
                w_copy(g + 2, slot, which).start()

    def attend(units):
        def scores(unit, buf):
            q, blocks, _ = unit
            top, row = None, 0
            for k, _, masked in blocks:
                t = _dot(k(), q())
                rows = t.shape[0]
                if masked:
                    seen = lax.broadcasted_iota(jnp.int32, t.shape, 0) <= lax.broadcasted_iota(jnp.int32, t.shape, 1)
                    t = jnp.where(seen, t, HIDDEN)
                buf[row : row + rows, :] = t
                most = t.reshape(rows // 8, 8, TILE).max(axis=0)
                top = most if top is None else jnp.maximum(top, most)
                row += rows
            return top.max(axis=0, keepdims=True)

        def mix(unit, buf, top):
            _, blocks, done = unit
            out, total, row = None, None, 0
            for _, v, _ in blocks:
                vals = v()
                for c in range(0, vals.shape[1], TILE):
                    p = jnp.exp2((buf[row : row + TILE, :] - top) * e)
                    add = p.reshape(TILE // 8, 8, TILE).sum(axis=0)
                    part = _dot(vals[:, c : c + TILE], p.astype(BF16))
                    total, out = (add, part) if out is None else (total + add, out + part)
                    row += TILE
            total = total.sum(axis=0, keepdims=True)
            done(out * (1 / total), top * scale + jnp.log(total))

        bufs = (s0, s1)
        top = scores(units[0], bufs[0])
        for u, unit in enumerate(units):
            after = scores(units[u + 1], bufs[(u + 1) % 2]) if u + 1 < len(units) else None
            mix(unit, bufs[u % 2], top)
            top = after

    halves = range(0, own, TILE)

    def far_units(g, h):
        def make(at):
            def done(o, lse):
                cross[g, h, :, at : at + TILE] = o.astype(BF16)
                for c in range(0, TILE, LANES):
                    stat_s[g, h, (at + c) // LANES : (at + c) // LANES + 1, :] = lse[:, c : c + LANES]
                if at + TILE == own:
                    s_move(g, h).start()
                    o_move(g, h).start()

            blocks = [(lambda: kb[g], lambda: vt[g], False), (lambda: kr[g], lambda: vr[g], False)]
            return lambda: cross[g, h, :, at : at + TILE], blocks, done

        return [make(at) for at in halves]

    def near_units(g, with_partner, with_direct, keep):
        def make(h, at):
            def done(o, lse):
                if keep:
                    ot[h, :, at : at + TILE] = o
                    lse_s[h : h + 1, at : at + TILE] = lse
                else:
                    obuf[at : at + TILE, h * HEAD : (h + 1) * HEAD] = o.astype(BF16).T

            blocks = [(lambda: kb[g, at : at + TILE, :], lambda: vt[g, :, at : at + TILE], True)]
            if at:
                blocks.append((lambda: kb[g, :at, :], lambda: vt[g, :, :at], False))
            if with_partner:
                blocks.append((lambda: kr[g], lambda: vr[g], False))
            if with_direct:
                blocks += [(lambda i=i: kd[i], lambda i=i: vd[i], False) for i in range(2)]
            return lambda: qt[g, h, :, at : at + TILE], blocks, done

        return [make(h, at) for h in range(per) for at in halves]

    def far_part(g):
        @pl.when(low & (g != DIRECT))
        def _():
            k_move(g).wait_recv()
            v_move(g).wait_recv()
            for h in range(per):
                q_move(g, h).wait_recv()
                attend(far_units(g, h))

    def forward():
        @pl.when(is_device(n - 2))
        def _():
            kd_move(1, kb.at[DIRECT], other).wait_recv()
            kd_move(1, kd.at[1], partner).start()

        @pl.when(is_device(n - 1))
        def _():
            kd_move(0, kb.at[DIRECT], other).wait_recv()
            vd_move(0, vt.at[DIRECT], other).wait_recv()
            kd_move(0, kd.at[0], partner).start()
            vd_move(0, vd.at[0], partner).start()

    def forward_late():
        @pl.when(is_device(0))
        def _():
            v_move(DIRECT).wait_recv()
            vd_move(1, vr.at[DIRECT], other).start()

    def near_part(g):
        direct = g == DIRECT

        @pl.when(is_device(1) & direct)
        def _():
            k_move(g).wait_recv()
            v_move(g).wait_recv()

        for right in (False, True):

            @pl.when(low & (odd == right))
            def _():
                attend(near_units(g, right, False, False))

        @pl.when(is_device(n - 1))
        def _():
            k_move(g).wait_recv()
            v_move(g).wait_recv()

        for right in (False, True):

            @pl.when(high & (odd == right) & jnp.logical_not(direct))
            def _():
                attend(near_units(g, right, False, True))

            @pl.when(high & (odd == right) & direct)
            def _():
                if right:
                    kd_move(1, kd.at[1], partner).wait_recv()
                else:
                    kd_move(0, kd.at[0], partner).wait_recv()
                    vd_move(0, vd.at[0], partner).wait_recv()
                vd_move(1, vd.at[1], partner).wait_recv()
                attend(near_units(g, right, True, False))

    def merge(g, h):
        s_move(g, h).wait_recv()
        o_move(g, h).wait_recv()
        mine = lse_s[h : h + 1, :]
        theirs = jnp.concatenate([stat_r[g, h, c : c + 1, :] for c in range(own // LANES)], axis=1)
        top = jnp.maximum(mine, theirs)
        wm, wt = jnp.exp(mine - top), jnp.exp(theirs - top)
        inv = 1 / (wm + wt)
        o = ot[h] * (wm * inv) + cross[g, h].astype(F32) * (wt * inv)
        obuf[:, h * HEAD : (h + 1) * HEAD] = o.astype(BF16).T

    cols = 2 * HEAD

    def y_copy(at):
        return pltpu.make_async_copy(ab.at[:, pl.ds(at, cols)], y_hbm.at[:, pl.ds(at, cols)], y_sem.at[at // cols])

    def out_part(j, g):
        slot = lax.rem(j, 2)
        wo_copy(g, slot).wait()

        def gather(rows):
            for at in range(0, d, cols):
                add = _dot(obuf[:, rows], wobuf[slot, rows, at : at + cols])
                acc[:, at : at + cols] = jnp.where(j > 0, acc[:, at : at + cols], 0.0) + add

        def close(rows):
            for at in range(0, d, cols):
                add = _dot(obuf[:, rows], wobuf[slot, rows, at : at + cols])
                ab[:, at : at + cols] = (ab[:, at : at + cols].astype(F32) + (acc[:, at : at + cols] + add)).astype(BF16)
                y_copy(at).start()

        whole, early, late = slice(0, per * HEAD), slice(0, (per - 1) * HEAD), slice((per - 1) * HEAD, per * HEAD)

        @pl.when(high & (g != DIRECT) & (j < last))
        def _():
            for h in range(per):
                merge(g, h)

        @pl.when(j < last)
        def _():
            gather(whole)

        @pl.when(j == last)
        def _():
            for r in range(4):
                x_copy(r).wait()

        @pl.when(low & (j == last))
        def _():
            close(whole)

        @pl.when(high & (j == last))
        def _():
            for h in range(per - 1):
                merge(g, h)
            gather(early)
            merge(g, per - 1)
            close(late)

        @pl.when(j + 2 < groups)
        def _():
            wo_copy(order(j + 2), slot).start()

    def step(i, _):
        j = i - LEAD
        g = order(j)

        @pl.when(i >= LEAD)
        def _():
            far_part(g)

        @pl.when(i < groups)
        def _():
            project_kv(i, False)
            project_q(i)

        @pl.when(i == LEAD)
        def _():
            forward()

        @pl.when(i == groups)
        def _():
            for r in range(4):
                x_copy(r).start()

        @pl.when(i >= LEAD)
        def _():
            near_part(g)

            @pl.when(j == LATE - 1)
            def _():
                forward_late()

            out_part(j, g)

        return 0

    lax.fori_loop(0, 2, lambda g, _: project_kv(g, True), None)
    for j in range(2):
        wo_copy(order(j), j).start()
    lax.fori_loop(0, 2, lambda g, _: project_q(g), None)
    lax.fori_loop(2, groups + LEAD, step, 0)

    def drain(g, _):
        usual = g != DIRECT

        @pl.when((me != n - 1) & usual | is_device(n - 2) | is_device(0))
        def _():
            k_move(g).wait_send()

        @pl.when(me != n - 1)
        def _():
            v_move(g).wait_send()

        @pl.when(usual)
        def _():
            for h in range(per):
                q_move(g, h).wait_send()

        @pl.when(low & usual)
        def _():
            for h in range(per):
                s_move(g, h).wait_send()

        return 0

    lax.fori_loop(0, groups, drain, 0)

    @pl.when(low)
    def _():
        kd_move(me, kb.at[DIRECT], other).wait_send()
        vd_move(me, vt.at[DIRECT], other).wait_send()

    @pl.when(is_device(0))
    def _():
        vd_move(1, vr.at[DIRECT], other).wait_send()

    @pl.when(is_device(n - 2))
    def _():
        kd_move(1, kd.at[1], partner).wait_send()

    @pl.when(is_device(n - 1))
    def _():
        kd_move(0, kd.at[0], partner).wait_send()
        vd_move(0, vd.at[0], partner).wait_send()

    for at in range(0, d, cols):
        y_copy(at).wait()


def _tables(n, own, half):
    rate = float(THETA) ** (-np.arange(half, dtype=np.float64) / half)
    near = np.arange(own, dtype=np.float64)[:, None] * rate
    far = (np.arange(n, dtype=np.float64) * own)[:, None] * rate
    return [np.stack([np.cos(t), np.sin(t)]).astype(np.float32) for t in (near, far)]


def solution(mesh):
    n = mesh.shape["sp"]

    def step(x, gain, wq, wk, wv, wo):
        own, d = x.shape
        groups = wk.shape[1] // HEAD
        per = wq.shape[1] // wk.shape[1]
        near, far = _tables(n, own, HEAD // 2)
        anyspace = pl.BlockSpec(memory_space=pl.ANY)
        vmem = pl.BlockSpec(memory_space=pltpu.VMEM)
        dma = pltpu.SemaphoreType.DMA
        return pl.pallas_call(
            functools.partial(_kernel, n, groups, per),
            out_shape=jax.ShapeDtypeStruct((own, d), BF16),
            in_specs=[anyspace, vmem, anyspace, vmem, anyspace, anyspace, anyspace, anyspace],
            out_specs=anyspace,
            scratch_shapes=[
                pltpu.VMEM((own, d), BF16),
                pltpu.VMEM((2, d, (per + 2) * HEAD), BF16),
                pltpu.VMEM((2, per * HEAD, d), BF16),
                pltpu.VMEM((groups, per, HEAD, own), BF16),
                pltpu.VMEM((groups, own, HEAD), BF16),
                pltpu.VMEM((groups, HEAD, own), BF16),
                pltpu.VMEM((groups, own, HEAD), BF16),
                pltpu.VMEM((groups, HEAD, own), BF16),
                pltpu.VMEM((2, own, HEAD), BF16),
                pltpu.VMEM((2, HEAD, own), BF16),
                pltpu.VMEM((groups, per, HEAD, own), BF16),
                pltpu.VMEM((groups, per, 8, LANES), F32),
                pltpu.VMEM((groups, per, 8, LANES), F32),
                pltpu.VMEM((own, d), F32),
                pltpu.VMEM((per, HEAD, own), F32),
                pltpu.VMEM((8, own), F32),
                pltpu.VMEM((own, per * HEAD), BF16),
                pltpu.VMEM((2, own, HEAD // 2), F32),
                pltpu.VMEM((4 * own, TILE), F32),
                pltpu.VMEM((4 * own, TILE), F32),
                dma((4,)), dma(()), dma((2, 3)), dma((2,)), dma((d // (2 * HEAD),)),
                dma((groups,)), dma((groups,)), dma((groups,)), dma((groups,)),
                dma((2,)), dma((2,)), dma((2,)), dma((2,)),
                dma((groups, per)), dma((groups, per)), dma((groups, per)), dma((groups, per)),
            ],
            compiler_params=pltpu.CompilerParams(collective_id=0, has_side_effects=True, vmem_limit_bytes=67043328),
            cost_estimate=pl.CostEstimate(flops=2 * own * d * HEAD * groups * (2 * per + 2), transcendentals=0,
                                          bytes_accessed=2 * d * HEAD * groups * (2 * per + 2)),
        )(x, gain, near, far, wq, wk, wv, wo)

    tokens, whole = P(("dp", "sp"), None), P(None, None)
    return jax.shard_map(
        step,
        mesh=mesh,
        in_specs=(tokens, P(None), whole, whole, whole, whole),
        out_specs=tokens,
        check_vma=False,
    )
```

```python
import functools

import jax
import jax.numpy as jnp
import numpy as np
from jax import lax
from jax.experimental import pallas as pl
from jax.experimental.pallas import tpu as pltpu
from jax.sharding import PartitionSpec as P

HEAD = 256
THETA = 10000
HIDDEN = -2e30
LOG2E = 1.4426950408889634
MESH = pl.DeviceIdType.MESH
TILE = 256
LANES = 128
DIRECT = 1
LEAD = 3
F32, BF16 = jnp.float32, jnp.bfloat16


def _dot(a, b):
    return lax.dot_general(a, b, (((1,), (0,)), ((), ())), preferred_element_type=F32)


def _kernel(n, groups, per, x_hbm, gain_ref, near_ref, far_ref, wq, wk, wv, wo, y_hbm,
            ab, wbuf, wobuf, qt, kb, vt, kr, vr, kd, vd, cross, stat_s, stat_r, acc, ot, lse_s, obuf, rope, s0, s1,
            x_sem, t_sem, w_sem, wo_sem, y_sem, ks_sem, kr_sem, vs_sem, vr_sem, kds_sem, kdr_sem, vds_sem, vdr_sem,
            cs_sem, cr_sem, ss_sem, sr_sem):
    own, d = ab.shape
    me = lax.axis_index("sp")
    partner = me + 1 - 2 * lax.rem(me, 2)
    other = n - 1 - me
    odd = lax.rem(me, 2) == 1
    low = me < n // 2
    high = jnp.logical_not(low)
    last = groups - 1

    def order(j):
        at = jnp.where(low, last, last - 2)
        return jnp.where(j == at, DIRECT, jnp.where((j >= DIRECT) & (j < at), j + 1, j))

    scale = HEAD**-0.5
    e = scale * LOG2E
    xrows = own // 4

    def x_copy(r):
        return pltpu.make_async_copy(x_hbm.at[pl.ds(r * xrows, xrows)], ab.at[pl.ds(r * xrows, xrows)], x_sem.at[r])

    def w_copy(g, slot, which):
        at = pl.ds(pl.multiple_of(g * HEAD, HEAD), HEAD)
        wide = pl.ds(pl.multiple_of(g * per * HEAD, per * HEAD), per * HEAD)
        src, into = [(wk.at[:, at], pl.ds(0, HEAD)), (wv.at[:, at], pl.ds(HEAD, HEAD)), (wq.at[:, wide], pl.ds(2 * HEAD, per * HEAD))][which]
        return pltpu.make_async_copy(src, wbuf.at[slot, :, into], w_sem.at[slot, which])

    def wo_copy(g, slot):
        return pltpu.make_async_copy(wo.at[pl.ds(pl.multiple_of(g * per * HEAD, HEAD), per * HEAD), :], wobuf.at[slot], wo_sem.at[slot])

    def remote(src, dst, s, r, to):
        return pltpu.make_async_remote_copy(src_ref=src, dst_ref=dst, send_sem=s, recv_sem=r, device_id={"sp": to}, device_id_type=MESH)

    def k_move(g):
        return remote(kb.at[g], kr.at[g], ks_sem.at[g], kr_sem.at[g], partner)

    def v_move(g):
        return remote(vt.at[g], vr.at[g], vs_sem.at[g], vr_sem.at[g], partner)

    def q_move(g, h, to):
        return remote(qt.at[g, h], cross.at[g, h], cs_sem.at[g, h], cr_sem.at[g, h], to)

    def o_move(g, h, to):
        return remote(cross.at[g, h], cross.at[g, h], cs_sem.at[g, h], cr_sem.at[g, h], to)

    def s_move(g, h, to):
        rows = pl.ds(0, own // LANES)
        return remote(stat_s.at[g, h, rows], stat_r.at[g, h, rows], ss_sem.at[g, h], sr_sem.at[g, h], to)

    def kd_move(slot, src, to):
        return remote(src, kd.at[slot], kds_sem.at[slot], kdr_sem.at[slot], to)

    def vd_move(slot, src, to):
        return remote(src, vd.at[slot], vds_sem.at[slot], vdr_sem.at[slot], to)

    def is_device(i):
        return me == i

    for r in range(4):
        x_copy(r).start()
    table = pltpu.make_async_copy(near_ref, rope, t_sem)
    table.start()
    w_copy(0, 0, 0).start()
    w_copy(0, 0, 1).start()

    barrier = pltpu.get_barrier_semaphore()
    for to in (partner, other):
        pl.semaphore_signal(barrier, inc=1, device_id={"sp": to}, device_id_type=MESH)

    gain = gain_ref[...].astype(F32).reshape(1, d)
    nr = 64
    for r in range(4):
        x_copy(r).wait()
        if r == 3:
            for g, which in ((1, 0), (1, 1), (0, 2), (1, 2)):
                w_copy(g, g, which).start()

        def norm(j, _):
            rows = pl.ds(pl.multiple_of(r * xrows + j * nr, nr), nr)
            wide = ab[rows, :].astype(F32)
            inv = lax.rsqrt(jnp.mean(wide * wide, -1, keepdims=True) + 1e-6)
            ab[rows, :] = (wide * inv * gain).astype(BF16)
            return 0

        lax.fori_loop(0, xrows // nr, norm, 0)

    table.wait()
    ca, sa = rope[0], rope[1]
    cf, sf = far_ref[0, pl.ds(me, 1), :], far_ref[1, pl.ds(me, 1), :]
    rope[0] = ca * cf - sa * sf
    rope[1] = sa * cf + ca * sf

    def turn(t):
        t = t.astype(BF16).astype(F32)
        half = HEAD // 2
        a, b = t[:, :half], t[:, half:]
        cos, sin = rope[0], rope[1]
        return jnp.concatenate([a * cos - b * sin, b * cos + a * sin], -1).astype(BF16)

    def project_kv(g, entering):
        slot = lax.rem(g, 2)
        w_copy(g, slot, 0).wait()
        w_copy(g, slot, 1).wait()
        kv = _dot(ab[...], wbuf[slot, :, : 2 * HEAD])
        kb[g] = turn(kv[:, :HEAD])
        vt[g] = kv[:, HEAD:].astype(BF16).T

        if entering:

            @pl.when(g == 0)
            def _():
                pl.semaphore_wait(barrier, 2)

        @pl.when((me != n - 1) & (g != DIRECT))
        def _():
            k_move(g).start()
            v_move(g).start()

        @pl.when(low & (g == DIRECT))
        def _():
            kd_move(me, kb.at[g], other).start()
            vd_move(me, vt.at[g], other).start()

        @pl.when(is_device(0) & (g == last))
        def _():
            k_move(DIRECT).start()
            v_move(DIRECT).start()

    def project_q(g):
        slot = lax.rem(g, 2)
        w_copy(g, slot, 2).wait()
        q = _dot(ab[...], wbuf[slot, :, 2 * HEAD :])
        for t in range(per):
            qt[g, t] = turn(q[:, t * HEAD : (t + 1) * HEAD]).T

        @pl.when(high & (g != DIRECT))
        def _():
            for t in range(per):
                q_move(g, t, other).start()

        @pl.when(is_device(n - 1) & (g == DIRECT))
        def _():
            for t in range(per):
                q_move(g, t, partner).start()

        @pl.when(g + 2 < groups)
        def _():
            for which in range(3):
                w_copy(g + 2, slot, which).start()

    def attend(units):
        def scores(unit, buf):
            q, blocks, _ = unit
            top, row = None, 0
            for k, _, masked in blocks:
                t = _dot(k(), q())
                rows = t.shape[0]
                if masked:
                    seen = lax.broadcasted_iota(jnp.int32, t.shape, 0) <= lax.broadcasted_iota(jnp.int32, t.shape, 1)
                    t = jnp.where(seen, t, HIDDEN)
                buf[row : row + rows, :] = t
                most = t.reshape(rows // 8, 8, TILE).max(axis=0)
                top = most if top is None else jnp.maximum(top, most)
                row += rows
            return top.max(axis=0, keepdims=True)

        def mix(unit, buf, top):
            _, blocks, done = unit
            out, total, row = None, None, 0
            for _, v, _ in blocks:
                vals = v()
                for c in range(0, vals.shape[1], TILE):
                    p = jnp.exp2((buf[row : row + TILE, :] - top) * e)
                    add = p.reshape(TILE // 8, 8, TILE).sum(axis=0)
                    part = _dot(vals[:, c : c + TILE], p.astype(BF16))
                    total, out = (add, part) if out is None else (total + add, out + part)
                    row += TILE
            total = total.sum(axis=0, keepdims=True)
            done(out * (1 / total), top * scale + jnp.log(total))

        bufs = (s0, s1)
        top = scores(units[0], bufs[0])
        for u, unit in enumerate(units):
            after = scores(units[u + 1], bufs[(u + 1) % 2]) if u + 1 < len(units) else None
            mix(unit, bufs[u % 2], top)
            top = after

    halves = range(0, own, TILE)

    def far_units(g, h, to, direct):
        def make(at):
            def done(o, lse):
                cross[g, h, :, at : at + TILE] = o.astype(BF16)
                for c in range(0, TILE, LANES):
                    stat_s[g, h, (at + c) // LANES : (at + c) // LANES + 1, :] = lse[:, c : c + LANES]
                if at + TILE == own:
                    s_move(g, h, to).start()
                    o_move(g, h, to).start()

            blocks = [(lambda: kb[g], lambda: vt[g], False)]
            if direct:
                blocks += [(lambda i=i: kd[i], lambda i=i: vd[i], False) for i in range(2)]
            else:
                blocks.append((lambda: kr[g], lambda: vr[g], False))
            return lambda: cross[g, h, :, at : at + TILE], blocks, done

        return [make(at) for at in halves]

    def near_units(g, with_partner, with_direct, keep):
        def make(h, at):
            def done(o, lse):
                if keep:
                    ot[h, :, at : at + TILE] = o
                    lse_s[h : h + 1, at : at + TILE] = lse
                else:
                    obuf[at : at + TILE, h * HEAD : (h + 1) * HEAD] = o.astype(BF16).T

            blocks = [(lambda: kb[g, at : at + TILE, :], lambda: vt[g, :, at : at + TILE], True)]
            if at:
                blocks.append((lambda: kb[g, :at, :], lambda: vt[g, :, :at], False))
            if with_partner:
                blocks.append((lambda: kr[g], lambda: vr[g], False))
            if with_direct:
                blocks += [(lambda i=i: kd[i], lambda i=i: vd[i], False) for i in range(2)]
            return lambda: qt[g, h, :, at : at + TILE], blocks, done

        return [make(h, at) for h in range(per) for at in halves]

    def far_part(g):
        @pl.when(low & (g != DIRECT))
        def _():
            k_move(g).wait_recv()
            v_move(g).wait_recv()
            for h in range(per):
                q_move(g, h, other).wait_recv()
                attend(far_units(g, h, other, False))

    def pass_on():
        @pl.when(is_device(n - 1))
        def _():
            kd_move(0, kb.at[DIRECT], other).wait_recv()
            vd_move(0, vt.at[DIRECT], other).wait_recv()
            kd_move(0, kd.at[0], partner).start()
            vd_move(0, vd.at[0], partner).start()

    def direct_part():
        @pl.when(is_device(n - 2))
        def _():
            for slot in range(2):
                kd_move(slot, kd.at[slot], partner).wait_recv()
                vd_move(slot, vd.at[slot], partner).wait_recv()
            for h in range(per):
                q_move(DIRECT, h, partner).wait_recv()
                attend(far_units(DIRECT, h, partner, True))

    def near_part(g):
        direct = g == DIRECT

        @pl.when(is_device(1) & direct)
        def _():
            k_move(g).wait_recv()
            v_move(g).wait_recv()

        for right in (False, True):

            @pl.when(low & (odd == right))
            def _():
                attend(near_units(g, right, False, False))

        @pl.when(is_device(n - 1) & jnp.logical_not(direct))
        def _():
            k_move(g).wait_recv()
            v_move(g).wait_recv()
            attend(near_units(g, True, False, True))

        @pl.when(high & (odd == direct))
        def _():
            attend(near_units(g, False, False, True))

        @pl.when(is_device(n - 2) & direct)
        def _():
            attend(near_units(g, False, True, False))

    def merge(g, h):
        s_move(g, h, other).wait_recv()
        o_move(g, h, other).wait_recv()
        mine = lse_s[h : h + 1, :]
        theirs = jnp.concatenate([stat_r[g, h, c : c + 1, :] for c in range(own // LANES)], axis=1)
        top = jnp.maximum(mine, theirs)
        wm, wt = jnp.exp(mine - top), jnp.exp(theirs - top)
        inv = 1 / (wm + wt)
        o = ot[h] * (wm * inv) + cross[g, h].astype(F32) * (wt * inv)
        obuf[:, h * HEAD : (h + 1) * HEAD] = o.astype(BF16).T

    cols = 2 * HEAD

    def y_copy(at):
        return pltpu.make_async_copy(ab.at[:, pl.ds(at, cols)], y_hbm.at[:, pl.ds(at, cols)], y_sem.at[at // cols])

    def out_part(j, g):
        slot = lax.rem(j, 2)
        wo_copy(g, slot).wait()

        def gather(rows):
            for at in range(0, d, cols):
                add = _dot(obuf[:, rows], wobuf[slot, rows, at : at + cols])
                acc[:, at : at + cols] = jnp.where(j > 0, acc[:, at : at + cols], 0.0) + add

        def close(rows):
            for at in range(0, d, cols):
                add = _dot(obuf[:, rows], wobuf[slot, rows, at : at + cols])
                ab[:, at : at + cols] = (ab[:, at : at + cols].astype(F32) + (acc[:, at : at + cols] + add)).astype(BF16)
                y_copy(at).start()

        whole, early, late = slice(0, per * HEAD), slice(0, (per - 1) * HEAD), slice((per - 1) * HEAD, per * HEAD)

        @pl.when((high & (g != DIRECT) | is_device(n - 1)) & (j < last))
        def _():
            for h in range(per):
                merge(g, h)

        @pl.when(j < last)
        def _():
            gather(whole)

        @pl.when(j == last)
        def _():
            for r in range(4):
                x_copy(r).wait()

        @pl.when(low & (j == last))
        def _():
            close(whole)

        @pl.when(high & (j == last))
        def _():
            for h in range(per - 1):
                merge(g, h)
            gather(early)
            merge(g, per - 1)
            close(late)

        @pl.when(j + 2 < groups)
        def _():
            wo_copy(order(j + 2), slot).start()

    def step(i, _):
        j = i - LEAD
        g = order(j)

        @pl.when(i >= LEAD)
        def _():
            far_part(g)

        @pl.when(i < groups)
        def _():
            project_kv(i, False)
            project_q(i)

        @pl.when(i == LEAD)
        def _():
            pass_on()

        @pl.when(i == LEAD + 1)
        def _():
            direct_part()

        @pl.when(i == groups)
        def _():
            for r in range(4):
                x_copy(r).start()

        @pl.when(i >= LEAD)
        def _():
            near_part(g)
            out_part(j, g)

        return 0

    lax.fori_loop(0, 2, lambda g, _: project_kv(g, True), None)
    for j in range(2):
        wo_copy(order(j), j).start()
    lax.fori_loop(0, 2, lambda g, _: project_q(g), None)
    lax.fori_loop(2, groups + LEAD, step, 0)

    def drain(g, _):
        usual = g != DIRECT

        @pl.when((me != n - 1) & usual | is_device(0))
        def _():
            k_move(g).wait_send()
            v_move(g).wait_send()

        @pl.when(usual | high)
        def _():
            for h in range(per):
                q_move(g, h, other).wait_send()

        @pl.when(low & usual | is_device(n - 2) & (g == DIRECT))
        def _():
            for h in range(per):
                s_move(g, h, other).wait_send()

        return 0

    lax.fori_loop(0, groups, drain, 0)

    @pl.when(low)
    def _():
        kd_move(me, kb.at[DIRECT], other).wait_send()
        vd_move(me, vt.at[DIRECT], other).wait_send()

    @pl.when(is_device(n - 1))
    def _():
        kd_move(0, kd.at[0], partner).wait_send()
        vd_move(0, vd.at[0], partner).wait_send()

    for at in range(0, d, cols):
        y_copy(at).wait()


def _tables(n, own, half):
    rate = float(THETA) ** (-np.arange(half, dtype=np.float64) / half)
    near = np.arange(own, dtype=np.float64)[:, None] * rate
    far = (np.arange(n, dtype=np.float64) * own)[:, None] * rate
    return [np.stack([np.cos(t), np.sin(t)]).astype(np.float32) for t in (near, far)]


def solution(mesh):
    n = mesh.shape["sp"]

    def step(x, gain, wq, wk, wv, wo):
        own, d = x.shape
        groups = wk.shape[1] // HEAD
        per = wq.shape[1] // wk.shape[1]
        near, far = _tables(n, own, HEAD // 2)
        anyspace = pl.BlockSpec(memory_space=pl.ANY)
        vmem = pl.BlockSpec(memory_space=pltpu.VMEM)
        dma = pltpu.SemaphoreType.DMA
        return pl.pallas_call(
            functools.partial(_kernel, n, groups, per),
            out_shape=jax.ShapeDtypeStruct((own, d), BF16),
            in_specs=[anyspace, vmem, anyspace, vmem, anyspace, anyspace, anyspace, anyspace],
            out_specs=anyspace,
            scratch_shapes=[
                pltpu.VMEM((own, d), BF16),
                pltpu.VMEM((2, d, (per + 2) * HEAD), BF16),
                pltpu.VMEM((2, per * HEAD, d), BF16),
                pltpu.VMEM((groups, per, HEAD, own), BF16),
                pltpu.VMEM((groups, own, HEAD), BF16),
                pltpu.VMEM((groups, HEAD, own), BF16),
                pltpu.VMEM((groups, own, HEAD), BF16),
                pltpu.VMEM((groups, HEAD, own), BF16),
                pltpu.VMEM((2, own, HEAD), BF16),
                pltpu.VMEM((2, HEAD, own), BF16),
                pltpu.VMEM((groups, per, HEAD, own), BF16),
                pltpu.VMEM((groups, per, 8, LANES), F32),
                pltpu.VMEM((groups, per, 8, LANES), F32),
                pltpu.VMEM((own, d), F32),
                pltpu.VMEM((per, HEAD, own), F32),
                pltpu.VMEM((8, own), F32),
                pltpu.VMEM((own, per * HEAD), BF16),
                pltpu.VMEM((2, own, HEAD // 2), F32),
                pltpu.VMEM((3 * own, TILE), F32),
                pltpu.VMEM((3 * own, TILE), F32),
                dma((4,)), dma(()), dma((2, 3)), dma((2,)), dma((d // (2 * HEAD),)),
                dma((groups,)), dma((groups,)), dma((groups,)), dma((groups,)),
                dma((2,)), dma((2,)), dma((2,)), dma((2,)),
                dma((groups, per)), dma((groups, per)), dma((groups, per)), dma((groups, per)),
            ],
            compiler_params=pltpu.CompilerParams(collective_id=0, has_side_effects=True, vmem_limit_bytes=67043328),
            cost_estimate=pl.CostEstimate(flops=2 * own * d * HEAD * groups * (2 * per + 2), transcendentals=0,
                                          bytes_accessed=2 * d * HEAD * groups * (2 * per + 2)),
        )(x, gain, near, far, wq, wk, wv, wo)

    tokens, whole = P(("dp", "sp"), None), P(None, None)
    return jax.shard_map(
        step,
        mesh=mesh,
        in_specs=(tokens, P(None), whole, whole, whole, whole),
        out_specs=tokens,
        check_vma=False,
    )
```

```python
import functools

import jax
import jax.numpy as jnp
import numpy as np
from jax import lax
from jax.experimental import pallas as pl
from jax.experimental.pallas import tpu as pltpu
from jax.sharding import PartitionSpec as P

HEAD = 256
THETA = 10000
HIDDEN = -2e30
LOG2E = 1.4426950408889634
MESH = pl.DeviceIdType.MESH
TILE = 256
LANES = 128
CHUNKS = 8
DIRECT = 1
LEAD = 3
F32, BF16 = jnp.float32, jnp.bfloat16


def _dot(a, b):
    return lax.dot_general(a, b, (((1,), (0,)), ((), ())), preferred_element_type=F32)


def _kernel(n, groups, per, x_hbm, gain_ref, near_ref, far_ref, wq, wk, wv, wo, y_hbm,
            ab, wbuf, wobuf, qt, kb, vt, kr, vr, kd, vd, cross, stat_s, stat_r, acc, ot, lse_s, obuf, rope, s0, s1,
            x_sem, t_sem, w_sem, wo_sem, y_sem, ks_sem, kr_sem, vs_sem, vr_sem, kds_sem, kdr_sem, vds_sem, vdr_sem,
            cs_sem, cr_sem, ss_sem, sr_sem):
    own, d = ab.shape
    me = lax.axis_index("sp")
    partner = me + 1 - 2 * lax.rem(me, 2)
    other = n - 1 - me
    odd = lax.rem(me, 2) == 1
    low = me < n // 2
    high = jnp.logical_not(low)
    last = groups - 1

    def order(j):
        at = jnp.where(low, last, last - 2)
        return jnp.where(j == at, DIRECT, jnp.where((j >= DIRECT) & (j < at), j + 1, j))

    scale = HEAD**-0.5
    e = scale * LOG2E
    xrows = own // 4

    def x_copy(r):
        return pltpu.make_async_copy(x_hbm.at[pl.ds(r * xrows, xrows)], ab.at[pl.ds(r * xrows, xrows)], x_sem.at[r])

    def w_copy(g, slot, which):
        at = pl.ds(pl.multiple_of(g * HEAD, HEAD), HEAD)
        wide = pl.ds(pl.multiple_of(g * per * HEAD, per * HEAD), per * HEAD)
        src, into = [(wk.at[:, at], pl.ds(0, HEAD)), (wv.at[:, at], pl.ds(HEAD, HEAD)), (wq.at[:, wide], pl.ds(2 * HEAD, per * HEAD))][which]
        return pltpu.make_async_copy(src, wbuf.at[slot, :, into], w_sem.at[slot, which])

    def wo_copy(g, slot):
        return pltpu.make_async_copy(wo.at[pl.ds(pl.multiple_of(g * per * HEAD, HEAD), per * HEAD), :], wobuf.at[slot], wo_sem.at[slot])

    def remote(src, dst, s, r, to):
        return pltpu.make_async_remote_copy(src_ref=src, dst_ref=dst, send_sem=s, recv_sem=r, device_id={"sp": to}, device_id_type=MESH)

    def k_move(g):
        return remote(kb.at[g], kr.at[g], ks_sem.at[g], kr_sem.at[g], partner)

    def v_move(g):
        return remote(vt.at[g], vr.at[g], vs_sem.at[g], vr_sem.at[g], partner)

    def q_move(g, h, to):
        return remote(qt.at[g, h], cross.at[g, h], cs_sem.at[g, h], cr_sem.at[g, h], to)

    def o_move(g, h, to):
        return remote(cross.at[g, h], cross.at[g, h], cs_sem.at[g, h], cr_sem.at[g, h], to)

    def s_move(g, h, to):
        rows = pl.ds(0, own // LANES)
        return remote(stat_s.at[g, h, rows], stat_r.at[g, h, rows], ss_sem.at[g, h], sr_sem.at[g, h], to)

    def kd_move(slot, src, to):
        return remote(src, kd.at[slot], kds_sem.at[slot], kdr_sem.at[slot], to)

    def vd_move(slot, src, to):
        return remote(src, vd.at[slot], vds_sem.at[slot], vdr_sem.at[slot], to)

    def is_device(i):
        return me == i

    for r in range(4):
        x_copy(r).start()
    table = pltpu.make_async_copy(near_ref, rope, t_sem)
    table.start()
    w_copy(0, 0, 0).start()
    w_copy(0, 0, 1).start()

    barrier = pltpu.get_barrier_semaphore()
    for to in (partner, other):
        pl.semaphore_signal(barrier, inc=1, device_id={"sp": to}, device_id_type=MESH)

    gain = gain_ref[...].astype(F32).reshape(1, d)
    nr = 64
    for r in range(4):
        x_copy(r).wait()
        if r == 3:
            for g, which in ((1, 0), (1, 1), (0, 2), (1, 2)):
                w_copy(g, g, which).start()

        def norm(j, _):
            rows = pl.ds(pl.multiple_of(r * xrows + j * nr, nr), nr)
            wide = ab[rows, :].astype(F32)
            inv = lax.rsqrt(jnp.mean(wide * wide, -1, keepdims=True) + 1e-6)
            ab[rows, :] = (wide * inv * gain).astype(BF16)
            return 0

        lax.fori_loop(0, xrows // nr, norm, 0)

    table.wait()
    ca, sa = rope[0], rope[1]
    cf, sf = far_ref[0, pl.ds(me, 1), :], far_ref[1, pl.ds(me, 1), :]
    rope[0] = ca * cf - sa * sf
    rope[1] = sa * cf + ca * sf

    def turn(t):
        t = t.astype(BF16).astype(F32)
        half = HEAD // 2
        a, b = t[:, :half], t[:, half:]
        cos, sin = rope[0], rope[1]
        return jnp.concatenate([a * cos - b * sin, b * cos + a * sin], -1).astype(BF16)

    def project_kv(g, entering):
        slot = lax.rem(g, 2)
        w_copy(g, slot, 0).wait()
        w_copy(g, slot, 1).wait()
        kv = _dot(ab[...], wbuf[slot, :, : 2 * HEAD])
        kb[g] = turn(kv[:, :HEAD])
        vt[g] = kv[:, HEAD:].astype(BF16).T

        if entering:

            @pl.when(g == 0)
            def _():
                pl.semaphore_wait(barrier, 2)

        @pl.when((me != n - 1) & (g != DIRECT))
        def _():
            k_move(g).start()
            v_move(g).start()

        @pl.when(low & (g == DIRECT))
        def _():
            kd_move(me, kb.at[g], other).start()
            vd_move(me, vt.at[g], other).start()

        @pl.when(is_device(0) & (g == last))
        def _():
            k_move(DIRECT).start()
            v_move(DIRECT).start()

    def project_q(g):
        slot = lax.rem(g, 2)
        w_copy(g, slot, 2).wait()
        q = _dot(ab[...], wbuf[slot, :, 2 * HEAD :])
        for t in range(per):
            qt[g, t] = turn(q[:, t * HEAD : (t + 1) * HEAD]).T

        @pl.when(high & (g != DIRECT))
        def _():
            for t in range(per):
                q_move(g, t, other).start()

        @pl.when(is_device(n - 1) & (g == DIRECT))
        def _():
            for t in range(per):
                q_move(g, t, partner).start()

        @pl.when(g + 2 < groups)
        def _():
            for which in range(3):
                w_copy(g + 2, slot, which).start()

    def attend(units):
        def scores(unit, buf):
            q, blocks, _ = unit
            top, row = None, 0
            for k, _, masked in blocks:
                t = _dot(k(), q())
                rows = t.shape[0]
                if masked:
                    seen = lax.broadcasted_iota(jnp.int32, t.shape, 0) <= lax.broadcasted_iota(jnp.int32, t.shape, 1)
                    t = jnp.where(seen, t, HIDDEN)
                buf[row : row + rows, :] = t
                most = t.reshape(rows // 8, 8, TILE).max(axis=0)
                top = most if top is None else jnp.maximum(top, most)
                row += rows
            return top.max(axis=0, keepdims=True)

        def mix(unit, buf, top):
            _, blocks, done = unit
            out, total, row = None, None, 0
            for _, v, _ in blocks:
                vals = v()
                for c in range(0, vals.shape[1], TILE):
                    p = jnp.exp2((buf[row : row + TILE, :] - top) * e)
                    add = p.reshape(TILE // 8, 8, TILE).sum(axis=0)
                    part = _dot(vals[:, c : c + TILE], p.astype(BF16))
                    total, out = (add, part) if out is None else (total + add, out + part)
                    row += TILE
            total = total.sum(axis=0, keepdims=True)
            done(out * (1 / total), top * scale + jnp.log(total))

        bufs = (s0, s1)
        top = scores(units[0], bufs[0])
        for u, unit in enumerate(units):
            after = scores(units[u + 1], bufs[(u + 1) % 2]) if u + 1 < len(units) else None
            mix(unit, bufs[u % 2], top)
            top = after

    halves = range(0, own, TILE)

    def far_units(g, h, to, direct):
        def make(at):
            def done(o, lse):
                cross[g, h, :, at : at + TILE] = o.astype(BF16)
                for c in range(0, TILE, LANES):
                    stat_s[g, h, (at + c) // LANES : (at + c) // LANES + 1, :] = lse[:, c : c + LANES]
                if at + TILE == own:
                    s_move(g, h, to).start()
                    o_move(g, h, to).start()

            blocks = [(lambda: kb[g], lambda: vt[g], False)]
            if direct:
                blocks += [(lambda i=i: kd[i], lambda i=i: vd[i], False) for i in range(2)]
            else:
                blocks.append((lambda: kr[g], lambda: vr[g], False))
            return lambda: cross[g, h, :, at : at + TILE], blocks, done

        return [make(at) for at in halves]

    def near_units(g, with_partner, with_direct, keep):
        def make(h, at):
            def done(o, lse):
                if keep:
                    ot[h, :, at : at + TILE] = o
                    lse_s[h : h + 1, at : at + TILE] = lse
                else:
                    obuf[at : at + TILE, h * HEAD : (h + 1) * HEAD] = o.astype(BF16).T

            blocks = [(lambda: kb[g, at : at + TILE, :], lambda: vt[g, :, at : at + TILE], True)]
            if at:
                blocks.append((lambda: kb[g, :at, :], lambda: vt[g, :, :at], False))
            if with_partner:
                blocks.append((lambda: kr[g], lambda: vr[g], False))
            if with_direct:
                blocks += [(lambda i=i: kd[i], lambda i=i: vd[i], False) for i in range(2)]
            return lambda: qt[g, h, :, at : at + TILE], blocks, done

        return [make(h, at) for h in range(per) for at in halves]

    def far_part(g):
        @pl.when(low & (g != DIRECT))
        def _():
            k_move(g).wait_recv()
            v_move(g).wait_recv()
            for h in range(per):
                q_move(g, h, other).wait_recv()
                attend(far_units(g, h, other, False))

    def pass_on():
        @pl.when(is_device(n - 1))
        def _():
            kd_move(0, kb.at[DIRECT], other).wait_recv()
            vd_move(0, vt.at[DIRECT], other).wait_recv()
            kd_move(0, kd.at[0], partner).start()
            vd_move(0, vd.at[0], partner).start()

    def direct_part():
        @pl.when(is_device(n - 2))
        def _():
            for slot in range(2):
                kd_move(slot, kd.at[slot], partner).wait_recv()
                vd_move(slot, vd.at[slot], partner).wait_recv()
            for h in range(per):
                q_move(DIRECT, h, partner).wait_recv()
                attend(far_units(DIRECT, h, partner, True))

    def near_part(g):
        direct = g == DIRECT

        @pl.when(is_device(1) & direct)
        def _():
            k_move(g).wait_recv()
            v_move(g).wait_recv()

        for right in (False, True):

            @pl.when(low & (odd == right))
            def _():
                attend(near_units(g, right, False, False))

        @pl.when(is_device(n - 1) & jnp.logical_not(direct))
        def _():
            k_move(g).wait_recv()
            v_move(g).wait_recv()
            attend(near_units(g, True, False, True))

        @pl.when(high & (odd == direct))
        def _():
            attend(near_units(g, False, False, True))

        @pl.when(is_device(n - 2) & direct)
        def _():
            attend(near_units(g, False, True, False))

    def merge(g, h):
        s_move(g, h, other).wait_recv()
        o_move(g, h, other).wait_recv()
        mine = lse_s[h : h + 1, :]
        theirs = jnp.concatenate([stat_r[g, h, c : c + 1, :] for c in range(own // LANES)], axis=1)
        top = jnp.maximum(mine, theirs)
        wm, wt = jnp.exp(mine - top), jnp.exp(theirs - top)
        inv = 1 / (wm + wt)
        o = ot[h] * (wm * inv) + cross[g, h].astype(F32) * (wt * inv)
        obuf[:, h * HEAD : (h + 1) * HEAD] = o.astype(BF16).T

    cols = 2 * HEAD

    def y_copy(at):
        return pltpu.make_async_copy(ab.at[:, pl.ds(at, cols)], y_hbm.at[:, pl.ds(at, cols)], y_sem.at[at // cols])

    def out_part(j, g):
        slot = lax.rem(j, 2)
        wo_copy(g, slot).wait()

        def gather(rows):
            for at in range(0, d, cols):
                add = _dot(obuf[:, rows], wobuf[slot, rows, at : at + cols])
                acc[:, at : at + cols] = jnp.where(j > 0, acc[:, at : at + cols], 0.0) + add

        def close(rows):
            for at in range(0, d, cols):
                add = _dot(obuf[:, rows], wobuf[slot, rows, at : at + cols])
                ab[:, at : at + cols] = (ab[:, at : at + cols].astype(F32) + (acc[:, at : at + cols] + add)).astype(BF16)
                y_copy(at).start()

        whole, early, late = slice(0, per * HEAD), slice(0, (per - 1) * HEAD), slice((per - 1) * HEAD, per * HEAD)

        @pl.when((high & (g != DIRECT) | is_device(n - 1)) & (j < last))
        def _():
            for h in range(per):
                merge(g, h)

        @pl.when(j < last)
        def _():
            gather(whole)

        @pl.when(j == last)
        def _():
            for r in range(4):
                x_copy(r).wait()

        @pl.when(low & (j == last))
        def _():
            close(whole)

        @pl.when(high & (j == last))
        def _():
            for h in range(per - 1):
                merge(g, h)
            gather(early)
            merge(g, per - 1)
            close(late)

        @pl.when(j + 2 < groups)
        def _():
            wo_copy(order(j + 2), slot).start()

    def step(i, _):
        j = i - LEAD
        g = order(j)

        @pl.when(i >= LEAD)
        def _():
            far_part(g)

        @pl.when(i < groups)
        def _():
            project_kv(i, False)
            project_q(i)

        @pl.when(i == LEAD)
        def _():
            pass_on()

        @pl.when(i == LEAD + 1)
        def _():
            direct_part()

        @pl.when(i == groups)
        def _():
            for r in range(4):
                x_copy(r).start()

        @pl.when(i >= LEAD)
        def _():
            near_part(g)
            out_part(j, g)

        return 0

    lax.fori_loop(0, 2, lambda g, _: project_kv(g, True), None)
    for j in range(2):
        wo_copy(order(j), j).start()
    lax.fori_loop(0, 2, lambda g, _: project_q(g), None)
    lax.fori_loop(2, groups + LEAD, step, 0)

    def drain(g, _):
        usual = g != DIRECT

        @pl.when((me != n - 1) & usual | is_device(0))
        def _():
            k_move(g).wait_send()
            v_move(g).wait_send()

        @pl.when(usual | high)
        def _():
            for h in range(per):
                q_move(g, h, other).wait_send()

        @pl.when(low & usual | is_device(n - 2) & (g == DIRECT))
        def _():
            for h in range(per):
                s_move(g, h, other).wait_send()

        return 0

    lax.fori_loop(0, groups, drain, 0)

    @pl.when(low)
    def _():
        kd_move(me, kb.at[DIRECT], other).wait_send()
        vd_move(me, vt.at[DIRECT], other).wait_send()

    @pl.when(is_device(n - 1))
    def _():
        kd_move(0, kd.at[0], partner).wait_send()
        vd_move(0, vd.at[0], partner).wait_send()

    for at in range(0, d, cols):
        y_copy(at).wait()


def _hand_over(src, dst, buf, in_sem, out_sem):
    rows = src.shape[0] // CHUNKS
    at = [pl.ds(i * rows, rows) for i in range(CHUNKS)]
    reads = [pltpu.make_async_copy(src.at[at[i]], buf.at[at[i]], in_sem.at[i]) for i in range(CHUNKS)]
    writes = [pltpu.make_async_copy(buf.at[at[i]], dst.at[at[i]], out_sem.at[i]) for i in range(CHUNKS)]
    for r in reads:
        r.start()
    for r, w in zip(reads, writes):
        r.wait()
        w.start()
    for w in writes:
        w.wait()


def _tables(n, own, half):
    rate = float(THETA) ** (-np.arange(half, dtype=np.float64) / half)
    near = np.arange(own, dtype=np.float64)[:, None] * rate
    far = (np.arange(n, dtype=np.float64) * own)[:, None] * rate
    return [np.stack([np.cos(t), np.sin(t)]).astype(np.float32) for t in (near, far)]


def solution(mesh):
    n = mesh.shape["sp"]

    def step(x, gain, wq, wk, wv, wo):
        own, d = x.shape
        groups = wk.shape[1] // HEAD
        per = wq.shape[1] // wk.shape[1]
        near, far = _tables(n, own, HEAD // 2)
        anyspace = pl.BlockSpec(memory_space=pl.ANY)
        vmem = pl.BlockSpec(memory_space=pltpu.VMEM)
        dma = pltpu.SemaphoreType.DMA
        y = pl.pallas_call(
            functools.partial(_kernel, n, groups, per),
            out_shape=jax.ShapeDtypeStruct((own, d), BF16),
            in_specs=[anyspace, vmem, anyspace, vmem, anyspace, anyspace, anyspace, anyspace],
            out_specs=anyspace,
            scratch_shapes=[
                pltpu.VMEM((own, d), BF16),
                pltpu.VMEM((2, d, (per + 2) * HEAD), BF16),
                pltpu.VMEM((2, per * HEAD, d), BF16),
                pltpu.VMEM((groups, per, HEAD, own), BF16),
                pltpu.VMEM((groups, own, HEAD), BF16),
                pltpu.VMEM((groups, HEAD, own), BF16),
                pltpu.VMEM((groups, own, HEAD), BF16),
                pltpu.VMEM((groups, HEAD, own), BF16),
                pltpu.VMEM((2, own, HEAD), BF16),
                pltpu.VMEM((2, HEAD, own), BF16),
                pltpu.VMEM((groups, per, HEAD, own), BF16),
                pltpu.VMEM((groups, per, 8, LANES), F32),
                pltpu.VMEM((groups, per, 8, LANES), F32),
                pltpu.VMEM((own, d), F32),
                pltpu.VMEM((per, HEAD, own), F32),
                pltpu.VMEM((8, own), F32),
                pltpu.VMEM((own, per * HEAD), BF16),
                pltpu.VMEM((2, own, HEAD // 2), F32),
                pltpu.VMEM((3 * own, TILE), F32),
                pltpu.VMEM((3 * own, TILE), F32),
                dma((4,)), dma(()), dma((2, 3)), dma((2,)), dma((d // (2 * HEAD),)),
                dma((groups,)), dma((groups,)), dma((groups,)), dma((groups,)),
                dma((2,)), dma((2,)), dma((2,)), dma((2,)),
                dma((groups, per)), dma((groups, per)), dma((groups, per)), dma((groups, per)),
            ],
            compiler_params=pltpu.CompilerParams(collective_id=0, has_side_effects=True, vmem_limit_bytes=67043328),
            cost_estimate=pl.CostEstimate(flops=2 * own * d * HEAD * groups * (2 * per + 2), transcendentals=0,
                                          bytes_accessed=2 * d * HEAD * groups * (2 * per + 2)),
        )(x, gain, near, far, wq, wk, wv, wo)
        return pl.pallas_call(
            _hand_over,
            out_shape=jax.ShapeDtypeStruct((own, d), BF16),
            in_specs=[anyspace],
            out_specs=anyspace,
            scratch_shapes=[pltpu.VMEM((own, d), BF16), dma((CHUNKS,)), dma((CHUNKS,))],
            compiler_params=pltpu.CompilerParams(vmem_limit_bytes=67043328),
        )(y)

    tokens, whole = P(("dp", "sp"), None), P(None, None)
    return jax.shard_map(
        step,
        mesh=mesh,
        in_specs=(tokens, P(None), whole, whole, whole, whole),
        out_specs=tokens,
        check_vma=False,
    )
```
